512 devices in a mesh: doc: 8 (over x, core), seq: 64 (over z, y).
Axes of the slice: x: 4, y: 4, z: 16, core: 2. Of those that a mesh axis runs over, the one named last changes fastest.
Arguments:
- queries: bfloat16 [65536, 1792], P(('doc', 'seq')), parts along dimension 0, may hold values from -5 to 5
- keys: bfloat16 [65536, 256], P(('doc', 'seq')), parts along dimension 0, may hold values from -5 to 5
- values: bfloat16 [65536, 256], P(('doc', 'seq')), parts along dimension 0, may hold values from -6 to 6
- doc_length: int32 [8], P('doc'), parts along dimension 0, may hold values from 4096 to 8192
- sink_pos: int32 [32], P('doc'), parts along dimension 0, may hold values from 0 to 127, as said below
Outputs:
- attended: bfloat16 [65536, 1792], P(('doc', 'seq')), parts along dimension 0
- row_lse: float32 [14, 65536], P(None, ('doc', 'seq')), parts along dimension 1
- sink_mass: float32 [14, 65536], P(None, ('doc', 'seq')), parts along dimension 1
- head_lse: float32 [112], P('doc'), parts along dimension 0
- head_sink: float32 [112], P('doc'), parts along dimension 0
The draws below stay inside these ranges and needn't reach their ends.
There are 8 independent parts, one for each index of `doc`. The reference program is written for one: setup_inputs(seed, part) draws one part's arguments, and reference() takes and returns one part's arrays. A program takes and returns all parts, laid end to end along the dimension named above; each array names one. Nothing has to cross between parts.
Inputs may be any that keep to these rules, and one draw needn't show every extreme that they name: `sink_pos`: 4 distinct positions within the document's first 128 tokens; positions 0 and 127 are always among them. Positions from doc_length up to 8192 are padding.
All inputs are finite; a program needn't handle non-finite values.
Results may differ from the reference program's by a relative error of at most 0.009.
Values may be sent and summed in bfloat16 or wider, within the bound.
A program may use at most 64 MiB of HBM per device.

```python
import jax
import jax.numpy as jnp
from jax import lax

QUERY_HEADS = 14
KEY_VALUE_HEADS = 2
HEAD_DIMENSION = 128
NSINK = 4
S_DEV = 128
PADDED_LENGTH = 8192


def draw_queries(key, part):
    query_group_width = QUERY_HEADS // KEY_VALUE_HEADS
    unsharded_result = jnp.clip(jax.random.normal(jax.random.fold_in(key, 11), (PADDED_LENGTH, KEY_VALUE_HEADS, query_group_width, HEAD_DIMENSION), jnp.float32), -5.0, 5.0)
    return unsharded_result.reshape(PADDED_LENGTH, QUERY_HEADS * HEAD_DIMENSION).astype(jnp.bfloat16)


def draw_keys(key, part):
    unsharded_result = jnp.clip(jax.random.normal(jax.random.fold_in(key, 13), (PADDED_LENGTH, KEY_VALUE_HEADS, HEAD_DIMENSION), jnp.float32), -5.0, 5.0)
    return unsharded_result.reshape(PADDED_LENGTH, KEY_VALUE_HEADS * HEAD_DIMENSION).astype(jnp.bfloat16)


def draw_sink_pos(key, part):
    order = jax.random.permutation(jax.random.fold_in(key, 17), S_DEV - 2)
    middle = order[:NSINK - 2].astype(jnp.int32) + 1
    first = jnp.zeros((1,), jnp.int32)
    last = jnp.full((1,), S_DEV - 1, jnp.int32)
    return jnp.concatenate([first, middle, last]).astype(jnp.int32)


def level_of(key, extent, split, low, top_value):
    loudness, own = 1.0, jax.random.fold_in(key, 6)
    for dim, shards_of in split:
        draws = jnp.exp(jax.random.uniform(jax.random.fold_in(own, dim), (shards_of,), jnp.float32, low / len(split), top_value / len(split)))
        loudness = loudness * jnp.repeat(draws, extent[dim] // shards_of).reshape([-1 if axis == dim else 1 for axis in range(len(extent))])
    return loudness


def scatter_about(rng, extent, deviation, most, pieces=(), kind=jnp.bfloat16):
    drawn = jax.random.normal(rng, extent, jnp.float32) * deviation
    if len(pieces) > 0:
        drawn = level_of(rng, extent, pieces, -0.22, 0.18) * drawn
    return jnp.clip(drawn, min=-most, max=most).astype(kind)


def setup_inputs(seed: int = 0, part: int = 0) -> dict:
    splits = jax.random.split(jax.random.key(seed), 6)
    own_keys = jax.random.split(jax.random.fold_in(splits[5], part), 6)
    return {
        "queries": draw_queries(jax.random.fold_in(jax.random.fold_in(splits[5], part), 71), part),
        "keys": draw_keys(jax.random.fold_in(jax.random.fold_in(splits[5], part), 71), part),
        "values": scatter_about(own_keys[2], (PADDED_LENGTH, KEY_VALUE_HEADS * HEAD_DIMENSION), 1.0, 6.0, ((0, 64),)),
        "doc_length": jax.random.randint(own_keys[3], (1,), PADDED_LENGTH // 2, PADDED_LENGTH + 1).astype(jnp.int32),
        "sink_pos": draw_sink_pos(jax.random.fold_in(jax.random.fold_in(splits[5], part), 71), part),
    }


def reference(queries, keys, values, doc_length, sink_pos):
    query_group_width = QUERY_HEADS // KEY_VALUE_HEADS
    length = doc_length[0]
    key_float = keys.reshape(PADDED_LENGTH, KEY_VALUE_HEADS, HEAD_DIMENSION).astype(jnp.float32)
    value_float = values.reshape(PADDED_LENGTH, KEY_VALUE_HEADS, HEAD_DIMENSION).astype(jnp.float32)
    key_pos = jnp.arange(PADDED_LENGTH, dtype=jnp.int32)
    is_sink = jnp.any(key_pos[:, None] == sink_pos[None, :], axis=1)
    rows_per_block = min(512, PADDED_LENGTH)
    block_count = PADDED_LENGTH // rows_per_block
    score_scale = HEAD_DIMENSION ** -0.5

    def one_block(block_index):
        first = (block_index * rows_per_block).astype(jnp.int32)
        query_float = lax.dynamic_slice_in_dim(queries, first, rows_per_block, 0)
        query_float = query_float.reshape(rows_per_block, KEY_VALUE_HEADS, query_group_width, HEAD_DIMENSION).astype(jnp.float32)
        scores = jnp.einsum("sgcd,pgd->gcsp", query_float, key_float, precision=lax.Precision.HIGHEST) * score_scale
        query_pos = first + jnp.arange(rows_per_block, dtype=jnp.int32)
        allowed = (key_pos[None, :] <= query_pos[:, None]) & (key_pos[None, :] < length)
        masked = jnp.where(allowed, scores, -jnp.inf)
        peak = jnp.max(masked, axis=-1, keepdims=True)
        row_lse = peak[..., 0] + jnp.log(jnp.sum(jnp.exp(masked - peak), axis=-1))
        probs = jnp.exp(masked - row_lse[..., None])
        sink_mass = jnp.sum(jnp.where(is_sink, probs, 0.0), axis=-1)
        rounded = lax.optimization_barrier(probs.astype(jnp.bfloat16)).astype(jnp.float32)
        attended = jnp.einsum("gcsp,pgd->sgcd", rounded, value_float, precision=lax.Precision.HIGHEST)
        attended = attended.reshape(rows_per_block, QUERY_HEADS * HEAD_DIMENSION)
        live_rows = query_pos < length
        attended = jnp.where(live_rows[:, None], attended, 0.0).astype(jnp.bfloat16)
        row_lse = jnp.where(live_rows[None, :], row_lse.reshape(QUERY_HEADS, rows_per_block), 0.0)
        sink_mass = jnp.where(live_rows[None, :], sink_mass.reshape(QUERY_HEADS, rows_per_block), 0.0)
        return attended, row_lse, sink_mass

    attended, row_lse, sink_mass = lax.map(one_block, jnp.arange(block_count, dtype=jnp.int32))
    attended = attended.reshape(PADDED_LENGTH, QUERY_HEADS * HEAD_DIMENSION)
    row_lse = row_lse.transpose(1, 0, 2).reshape(QUERY_HEADS, PADDED_LENGTH)
    sink_mass = sink_mass.transpose(1, 0, 2).reshape(QUERY_HEADS, PADDED_LENGTH)
    doc_count = length.astype(jnp.float32)
    head_lse = jnp.sum(row_lse, axis=1) / doc_count
    head_sink = jnp.sum(sink_mass, axis=1) / doc_count
    return (attended, row_lse, sink_mass, head_lse, head_sink)
```

```python
import functools

import jax
import jax.numpy as jnp
from jax import lax
from jax.experimental import pallas as pl
from jax.experimental.pallas import tpu as pltpu
from jax.sharding import PartitionSpec as P

MESH = pl.DeviceIdType.MESH
D = 128
R = 128
NY = 4
HG = 7
CW = HG * D
SCALE = D**-0.5
LC = SCALE * 1.4426950408889634
LOW = -(2.0**60)


def gray(i):
    return i + (i // 2) * (1 - 2 * (i % 2))


def kernel(
    NZ,
    len_ref,
    sink_ref,
    q_hbm,
    k_hbm,
    v_hbm,
    out_ref,
    lse_ref,
    mass_ref,
    hl_ref,
    hs_ref,
    qbuf,
    qx,
    kbuf,
    vbuf,
    kx,
    vx,
    ebuf,
    m_ref,
    acc_ref,
    osend,
    xsend,
    orecv,
    xrecv,
    xs_ref,
    pk_ref,
    ysum,
    zsum,
    loc_sem,
    qs_sem,
    qr_sem,
    xk_sem,
    kr_sem,
    vr_sem,
    kus,
    vus,
    kds,
    vds,
    os_sem,
    or_sem,
    ss_sem,
    sr_sem,
    ys_sem,
    yr_sem,
    zs_sem,
    zr_sem,
):
    NU = NZ // 2
    ND = NU - 1
    KD = NU - 2
    NST = NU // 2
    s = lax.axis_index("seq")
    z = s // NY
    y = s % NY
    g = y % 2
    b = y // 2

    def dev(zz, yy):
        return {"seq": zz * NY + yy}

    def lanes(ref, start, size):
        return ref.at[:, pl.ds(pl.multiple_of(start, 128), size)]

    c0 = pltpu.make_async_copy(lanes(k_hbm, g * D, D), kbuf.at[pl.ds(pl.multiple_of(g * R, R), R), :], loc_sem.at[0])
    c1 = pltpu.make_async_copy(lanes(v_hbm, g * D, D), vbuf.at[pl.ds(pl.multiple_of(g * R, R), R), :], loc_sem.at[1])
    c2 = pltpu.make_async_copy(lanes(k_hbm, (1 - g) * D, D), kx, loc_sem.at[2])
    c3 = pltpu.make_async_copy(lanes(v_hbm, (1 - g) * D, D), vx, loc_sem.at[3])
    c4 = pltpu.make_async_copy(lanes(q_hbm, (1 - g) * CW, CW), qx, loc_sem.at[4])
    c5 = pltpu.make_async_copy(lanes(q_hbm, g * CW, CW), qbuf.at[y], loc_sem.at[5])
    for c in (c0, c1, c2, c3, c4, c5):
        c.start()

    barrier = pltpu.get_barrier_semaphore()

    def greet_z(i, _):
        pl.semaphore_signal(barrier, inc=1, device_id=dev((z + i) % NZ, y), device_id_type=MESH)
        return 0

    def greet_y(i, _):
        pl.semaphore_signal(barrier, inc=1, device_id=dev(z, (y + i) % NY), device_id_type=MESH)
        return 0

    lax.fori_loop(1, NY, greet_y, 0)
    lax.fori_loop(1, NZ, greet_z, 0)

    lane = lax.broadcasted_iota(jnp.int32, (2 * R, D), 1)
    row = lax.broadcasted_iota(jnp.int32, (2 * R, D), 0)
    plain = jnp.where(lane < 64, 1.0, 0.0).astype(jnp.bfloat16)

    def fill(i, _):
        ebuf[pl.ds(pl.multiple_of(i * 2 * R, 2 * R), 2 * R), :] = plain
        return 0

    lax.fori_loop(0, NZ, fill, 0)
    kpos = row + b * 2 * R
    hit = kpos == sink_ref[0]
    for n in range(1, 4):
        hit = hit | (kpos == sink_ref[n])
    first = jnp.where(z < NU + 1, z, NZ + 1 - z)
    ebuf[pl.ds(pl.multiple_of(first * 2 * R, 2 * R), 2 * R), :] = jnp.where(
        (lane < 64) | hit, 1.0, 0.0
    ).astype(jnp.bfloat16)

    for c in (c0, c1, c2, c3, c4, c5):
        c.wait()
    pl.semaphore_wait(barrier, NY - 1 + NZ - 1)

    def cell(ref, slot, c):
        return ref.at[pl.ds(pl.multiple_of(slot * (2 * R) + c * R, R), R), :]

    def up_slot(zz, j):
        return j + jnp.maximum(0, j - (NZ - zz))

    def down_slot(zz, j):
        return jnp.where(zz + j >= NZ, 2 * j + 1 - (NZ - zz), NZ + j)

    def pair(slot, tslot, c, ss, vs, j, zt, yt):
        return (
            pltpu.make_async_remote_copy(
                src_ref=cell(kbuf, slot, c),
                dst_ref=cell(kbuf, tslot, c),
                send_sem=ss.at[j, c],
                recv_sem=kr_sem.at[tslot, c],
                device_id=dev(zt, yt),
                device_id_type=MESH,
            ),
            pltpu.make_async_remote_copy(
                src_ref=cell(vbuf, slot, c),
                dst_ref=cell(vbuf, tslot, c),
                send_sem=vs.at[j, c],
                recv_sem=vr_sem.at[tslot, c],
                device_id=dev(zt, yt),
                device_id_type=MESH,
            ),
        )

    def up(slot, c, j):
        return pair(slot, up_slot(z + 1, j + 1), c, kus, vus, j, (z + 1) % NZ, y)

    def down(slot, c, j):
        zt = (z + NZ - 1) % NZ
        return pair(slot, down_slot(zt, j + 1), c, kds, vds, j, zt, y)

    def start_up(slot, c, j):
        @pl.when((j < NU) & (z < NZ - 1) & (z >= j))
        def _():
            for d in up(slot, c, j):
                d.start()

    def start_down(slot, c, j):
        @pl.when((j < ND) & ((z + j) % NZ <= KD))
        def _():
            for d in down(slot, c, j):
                d.start()

    start_up(0, g, 0)
    start_down(0, g, 0)

    yp = y + 1 - 2 * g
    to_pair = (
        pltpu.make_async_remote_copy(
            src_ref=kx, dst_ref=cell(kbuf, 0, g), send_sem=xk_sem.at[0], recv_sem=kr_sem.at[0, g],
            device_id=dev(z, yp), device_id_type=MESH,
        ),
        pltpu.make_async_remote_copy(
            src_ref=vx, dst_ref=cell(vbuf, 0, g), send_sem=xk_sem.at[1], recv_sem=vr_sem.at[0, g],
            device_id=dev(z, yp), device_id_type=MESH,
        ),
    )
    for d in to_pair:
        d.start()

    def q_copy(i):
        src = qbuf.at[y] if i == 2 else qx
        return pltpu.make_async_remote_copy(
            src_ref=src, dst_ref=qbuf.at[y], send_sem=qs_sem.at[i], recv_sem=qr_sem.at[y],
            device_id=dev(z, (y + i) % NY), device_id_type=MESH,
        )

    for i in (1, 3, 2):
        q_copy(i).start()

    def wait_cell(slot, c):
        for ref, sem in ((kbuf, kr_sem), (vbuf, vr_sem)):
            pltpu.make_async_remote_copy(
                src_ref=cell(ref, slot, c), dst_ref=cell(ref, slot, c), send_sem=xk_sem.at[0],
                recv_sem=sem.at[slot, c], device_id=dev(z, yp), device_id_type=MESH,
            ).wait_recv()

    def wait_q(t):
        pltpu.make_async_remote_copy(
            src_ref=qx, dst_ref=qbuf.at[t], send_sem=qs_sem.at[0], recv_sem=qr_sem.at[t],
            device_id=dev(z, yp), device_id_type=MESH,
        ).wait_recv()

    wait_cell(0, 1 - g)
    start_up(0, 1 - g, 0)
    start_down(0, 1 - g, 0)

    def poll(e):
        j = e // 2 + 1
        c = (g + e) % 2

        @pl.when(z >= j)
        def _():
            slot = up_slot(z, j)
            wait_cell(slot, c)
            start_up(slot, c, j)

        @pl.when((j <= ND) & ((z + j) % NZ <= KD))
        def _():
            slot = down_slot(z, j)
            wait_cell(slot, c)
            start_down(slot, c, j)

    def scores(t, h, k):
        return lax.dot_general(
            qbuf[t, :, h * D : (h + 1) * D], k, (((1,), (1,)), ((), ())), preferred_element_type=jnp.float32
        )

    def weigh(sc, mn):
        mc = mn * LC
        cols = [jnp.exp2(sc[:, n * D : (n + 1) * D] * LC - mc) for n in range(sc.shape[1] // D)]
        return jnp.concatenate(cols, axis=1).astype(jnp.bfloat16)

    def mix(p, ve):
        return lax.dot_general(p, ve, (((1,), (0,)), ((), ())), preferred_element_type=jnp.float32)

    qi = lax.broadcasted_iota(jnp.int32, (R, 2 * R), 0)
    ki = lax.broadcasted_iota(jnp.int32, (R, 2 * R), 1)

    def attend_own(t):
        k = kbuf[0 : 2 * R, :]
        ve = jnp.concatenate([vbuf[0 : 2 * R, :], ebuf[0 : 2 * R, :]], axis=1)
        ok = ki + b * 2 * R <= qi + t * R
        sc = [jnp.where(ok, scores(t, h, k), LOW) for h in range(HG)]
        for h in range(HG):
            mn = jnp.broadcast_to(jnp.max(sc[h], axis=1, keepdims=True), (R, D))
            m_ref[t, h] = mn
            acc_ref[t, h] = mix(weigh(sc[h], mn), ve)

    def attend(t, base, n):
        rows = pl.ds(pl.multiple_of(base, 2 * R), n * 2 * R)
        k = kbuf[rows, :]
        ve = jnp.concatenate([vbuf[rows, :], ebuf[rows, :]], axis=1)
        sc = [scores(t, h, k) for h in range(HG)]
        for h in range(HG):
            mo = m_ref[t, h]
            mn = jnp.maximum(mo, jnp.max(sc[h], axis=1, keepdims=True))
            al = jnp.exp2((mo - mn) * LC)
            pv = mix(weigh(sc[h], mn), ve)
            acc_ref[t, h] = acc_ref[t, h] * jnp.concatenate([al, al], axis=1) + pv
            m_ref[t, h] = mn

    def own_step(i, _):
        t = (y + gray(i)) % NY

        @pl.when(i > 0)
        def _():
            wait_q(t)

        attend_own(t)
        poll(i)
        return 0

    lax.fori_loop(0, NY, own_step, 0)

    def have(st):
        return jnp.minimum(2 * st, z) + jnp.maximum(0, jnp.minimum(2 * st, ND) - (NZ - z) + 1)

    lane1 = lax.broadcasted_iota(jnp.int32, (R, D), 1)

    def finish(t, gi):
        x = jnp.zeros((R, D), jnp.float32)
        for h in range(HG):
            a = acc_ref[t, h]
            total = jnp.broadcast_to(a[:, D : D + 1], (R, D))
            mass = jnp.broadcast_to(a[:, D + 64 : D + 65], (R, D))
            inv = 1.0 / total
            osend[gi, :, h * D : (h + 1) * D] = (a[:, :D] * inv).astype(jnp.bfloat16)
            x = jnp.where(lane1 == h, m_ref[t, h] * SCALE + jnp.log(total), x)
            x = jnp.where(lane1 == 8 + h, mass * inv, x)
        xs_ref[...] = x.T
        xsend[gi] = xs_ref[0:16, :]

    def back(gi):
        t = (y + gi) % NY
        return (
            pltpu.make_async_remote_copy(
                src_ref=xsend.at[gi], dst_ref=xrecv.at[y], send_sem=ss_sem.at[gi], recv_sem=sr_sem.at[y],
                device_id=dev(z, t), device_id_type=MESH,
            ),
            pltpu.make_async_remote_copy(
                src_ref=osend.at[gi], dst_ref=orecv.at[y], send_sem=os_sem.at[gi], recv_sem=or_sem.at[y],
                device_id=dev(z, t), device_id_type=MESH,
            ),
        )

    def stage_step(it, _):
        st = it // NY + 1
        i = it % NY
        last = st == NST
        before = have(st - 1)
        count = have(st) - before
        gi = gray(jnp.where(last, NY - 1 - i, i))
        t = (y + gi) % NY
        for n in range(1, 5):

            @pl.when(count == n)
            def _():
                attend(t, (before + 1) * 2 * R, n)

        @pl.when(st < NST)
        def _():
            poll(NY * st + i)

        @pl.when(last)
        def _():
            finish(t, gi)

            @pl.when(gi > 0)
            def _():
                for d in back(gi):
                    d.start()

        return 0

    lax.fori_loop(0, NST * NY, stage_step, 0)

    xrecv[y] = xsend[0]
    for i in range(1, NY):
        yy = (y + i) % NY
        pltpu.make_async_remote_copy(
            src_ref=xsend.at[0], dst_ref=xrecv.at[yy], send_sem=ss_sem.at[0], recv_sem=sr_sem.at[yy],
            device_id=dev(z, yp), device_id_type=MESH,
        ).wait_recv()
    pos = s * R + lax.broadcasted_iota(jnp.int32, (8, D), 1)
    live = pos < len_ref[0]
    pk_ref[...] = jnp.zeros_like(pk_ref)
    for gg in range(2):
        xa, xb = xrecv[gg], xrecv[2 + gg]
        la, lb = xa[0:8], xb[0:8]
        top = jnp.maximum(la, lb)
        ea, eb = jnp.exp(la - top), jnp.exp(lb - top)
        tot = ea + eb
        wa, wb = ea / tot, eb / tot
        lse = jnp.where(live, top + jnp.log(tot), 0.0)
        mass = jnp.where(live, wa * xa[8:16] + wb * xb[8:16], 0.0)
        lse_ref[gg * HG : (gg + 1) * HG, :] = lse[0:HG]
        mass_ref[gg * HG : (gg + 1) * HG, :] = mass[0:HG]
        pk_ref[32 + 16 * gg : 40 + 16 * gg, :] = jnp.where(live, wa, 0.0)
        pk_ref[40 + 16 * gg : 48 + 16 * gg, :] = jnp.where(live, wb, 0.0)
    pk_ref[0 : 2 * HG, :] = lse_ref[...]
    pk_ref[16 : 16 + 2 * HG, :] = mass_ref[...]
    xs_ref[...] = pk_ref[...].T
    ysum[y] = jnp.broadcast_to(jnp.sum(xs_ref[...], axis=0, keepdims=True), (8, D))

    def sum_y(i):
        return pltpu.make_async_remote_copy(
            src_ref=ysum.at[y], dst_ref=ysum.at[y], send_sem=ys_sem.at[i], recv_sem=yr_sem.at[y],
            device_id=dev(z, (y + i) % NY), device_id_type=MESH,
        )

    for i in range(1, NY):
        sum_y(i).start()
    for i in range(1, NY):
        yy = (y + i) % NY
        pltpu.make_async_remote_copy(
            src_ref=ysum.at[y], dst_ref=ysum.at[yy], send_sem=ys_sem.at[0], recv_sem=yr_sem.at[yy],
            device_id=dev(z, yp), device_id_type=MESH,
        ).wait_recv()
    zsum[z] = ysum[0] + ysum[1] + ysum[2] + ysum[3]

    def sum_z(i):
        return pltpu.make_async_remote_copy(
            src_ref=zsum.at[z], dst_ref=zsum.at[z], send_sem=zs_sem.at[i], recv_sem=zr_sem.at[z],
            device_id=dev((z + i) % NZ, y), device_id_type=MESH,
        )

    def sum_z_start(i, _):
        sum_z(i).start()
        return 0

    lax.fori_loop(1, NZ, sum_z_start, 0)

    orecv[y] = osend[0]
    for i in range(1, NY):
        yy = (y + i) % NY
        pltpu.make_async_remote_copy(
            src_ref=osend.at[0], dst_ref=orecv.at[yy], send_sem=os_sem.at[0], recv_sem=or_sem.at[yy],
            device_id=dev(z, yp), device_id_type=MESH,
        ).wait_recv()
    for gg in range(2):
        for h in range(HG):
            at = 32 + 16 * gg + h
            cols = slice(h * D, (h + 1) * D)
            o = xs_ref[:, at : at + 1] * orecv[gg, :, cols].astype(jnp.float32)
            o = o + xs_ref[:, at + 8 : at + 9] * orecv[2 + gg, :, cols].astype(jnp.float32)
            out_ref[:, gg * CW + h * D : gg * CW + (h + 1) * D] = o.astype(jnp.bfloat16)

    def sum_z_wait(i, _):
        zz = (z + i) % NZ
        pltpu.make_async_remote_copy(
            src_ref=zsum.at[z], dst_ref=zsum.at[zz], send_sem=zs_sem.at[0], recv_sem=zr_sem.at[zz],
            device_id=dev(z, yp), device_id_type=MESH,
        ).wait_recv()
        return 0

    lax.fori_loop(1, NZ, sum_z_wait, 0)
    total = zsum[0]
    for i in range(1, NZ):
        total = total + zsum[i]
    mean = total[0:1, :] / len_ref[0].astype(jnp.float32)
    hl_ref[...] = mean[:, 0 : 2 * HG]
    hs_ref[...] = mean[:, 16 : 16 + 2 * HG]

    for c in range(2):
        for j in range(NU):

            @pl.when((z < NZ - 1) & (z >= j))
            def _():
                for d in up(0, c, j):
                    d.wait_send()

        for j in range(ND):

            @pl.when((z + j) % NZ <= KD)
            def _():
                for d in down(0, c, j):
                    d.wait_send()

    for d in to_pair:
        d.wait_send()
    for i in (1, 3, 2):
        q_copy(i).wait_send()
        sum_y(i).wait_send()
        for d in back(i):
            d.wait_send()

    def sum_z_sent(i, _):
        sum_z(i).wait_send()
        return 0

    lax.fori_loop(1, NZ, sum_z_sent, 0)


def body(queries, keys, values, doc_length, sink_pos):
    NZ = lax.axis_size("seq") // NY
    NU = NZ // 2
    cells = NZ + NU
    f32, bf16 = jnp.float32, jnp.bfloat16
    vm, dma = pltpu.VMEM, pltpu.SemaphoreType.DMA
    out, lse, mass, hl, hs = pl.pallas_call(
        functools.partial(kernel, NZ),
        out_shape=(
            jax.ShapeDtypeStruct((R, 2 * CW), bf16),
            jax.ShapeDtypeStruct((2 * HG, R), f32),
            jax.ShapeDtypeStruct((2 * HG, R), f32),
            jax.ShapeDtypeStruct((1, 2 * HG), f32),
            jax.ShapeDtypeStruct((1, 2 * HG), f32),
        ),
        in_specs=[
            pl.BlockSpec(memory_space=pltpu.SMEM),
            pl.BlockSpec(memory_space=pltpu.SMEM),
            pl.BlockSpec(memory_space=pl.ANY),
            pl.BlockSpec(memory_space=pl.ANY),
            pl.BlockSpec(memory_space=pl.ANY),
        ],
        out_specs=(pl.BlockSpec(memory_space=vm),) * 5,
        scratch_shapes=[
            vm((NY, R, CW), bf16),
            vm((R, CW), bf16),
            vm((cells * 2 * R, D), bf16),
            vm((cells * 2 * R, D), bf16),
            vm((R, D), bf16),
            vm((R, D), bf16),
            vm((NZ * 2 * R, D), bf16),
            vm((NY, HG, R, D), f32),
            vm((NY, HG, R, 2 * D), f32),
            vm((NY, R, CW), bf16),
            vm((NY, 16, R), f32),
            vm((NY, R, CW), bf16),
            vm((NY, 16, R), f32),
            vm((R, D), f32),
            vm((D, R), f32),
            vm((NY, 8, D), f32),
            vm((NZ, 8, D), f32),
            dma((6,)),
            dma((NY,)),
            dma((NY,)),
            dma((2,)),
            dma((cells, 2)),
            dma((cells, 2)),
            dma((NU, 2)),
            dma((NU, 2)),
            dma((NU, 2)),
            dma((NU, 2)),
            dma((NY,)),
            dma((NY,)),
            dma((NY,)),
            dma((NY,)),
            dma((NY,)),
            dma((NY,)),
            dma((NZ,)),
            dma((NZ,)),
        ],
        compiler_params=pltpu.CompilerParams(
            collective_id=0, has_side_effects=True, vmem_limit_bytes=56 * 2**20
        ),
    )(doc_length, sink_pos, queries, keys, values)
    return out, lse, mass, hl.reshape(2 * HG), hs.reshape(2 * HG)


def solution(mesh):
    rows = P(("doc", "seq"), None)
    return jax.shard_map(
        body,
        mesh=mesh,
        in_specs=(rows, rows, rows, P("doc"), P("doc")),
        out_specs=(rows, P(None, ("doc", "seq")), P(None, ("doc", "seq")), P("doc"), P("doc")),
        check_vma=False,
    )
```

```python
import functools

import jax
import jax.numpy as jnp
from jax import lax
from jax.experimental import pallas as pl
from jax.experimental.pallas import tpu as pltpu
from jax.sharding import PartitionSpec as P

MESH = pl.DeviceIdType.MESH
D = 128
R = 128
NY = 4
HG = 7
CW = HG * D
SCALE = D**-0.5
LC = SCALE * 1.4426950408889634
LOW = -(2.0**60)


def gray(i):
    return i + (i // 2) * (1 - 2 * (i % 2))


def kernel(
    NZ,
    len_hbm,
    sink_hbm,
    q_hbm,
    k_hbm,
    v_hbm,
    out_hbm,
    lse_hbm,
    mass_hbm,
    hl_hbm,
    hs_hbm,
    len_ref,
    sink_ref,
    lse_ref,
    mass_ref,
    hl_ref,
    hs_ref,
    qbuf,
    qx,
    kbuf,
    vbuf,
    kx,
    vx,
    ebuf,
    m_ref,
    acc_ref,
    osend,
    orecv,
    obuf,
    xrecv,
    xs_ref,
    pk_ref,
    zsum,
    loc_sem,
    qs_sem,
    qr_sem,
    xk_sem,
    kr_sem,
    vr_sem,
    kus,
    vus,
    kds,
    vds,
    os_sem,
    or_sem,
    ss_sem,
    sr_sem,
    zs_sem,
    zr_sem,
    hello,
):
    NU = NZ // 2
    ND = NU - 1
    KD = NU - 2
    NST = NU // 2
    s = lax.axis_index("seq")
    z = s // NY
    y = s % NY
    g = y % 2
    b = y // 2

    def dev(zz, yy):
        return {"seq": zz * NY + yy}

    def lanes(ref, start, size):
        return ref.at[:, pl.ds(pl.multiple_of(start, 128), size)]

    barrier = pltpu.get_barrier_semaphore()

    beside = ((z + 1) % NZ, (z + NZ - 1) % NZ)
    for zz in beside:
        pl.semaphore_signal(barrier, inc=1, device_id=dev(zz, y), device_id_type=MESH)
    for i in range(1, NY):
        pl.semaphore_signal(barrier, inc=1, device_id=dev(z, (y + i) % NY), device_id_type=MESH)

    c0 = pltpu.make_async_copy(lanes(k_hbm, g * D, D), kbuf.at[pl.ds(pl.multiple_of(g * R, R), R), :], loc_sem.at[0])
    c1 = pltpu.make_async_copy(lanes(v_hbm, g * D, D), vbuf.at[pl.ds(pl.multiple_of(g * R, R), R), :], loc_sem.at[1])
    c2 = pltpu.make_async_copy(lanes(k_hbm, (1 - g) * D, D), kx, loc_sem.at[2])
    c3 = pltpu.make_async_copy(lanes(v_hbm, (1 - g) * D, D), vx, loc_sem.at[3])
    c4 = pltpu.make_async_copy(lanes(q_hbm, (1 - g) * CW, CW), qx, loc_sem.at[4])
    c5 = pltpu.make_async_copy(lanes(q_hbm, g * CW, CW), qbuf.at[y], loc_sem.at[5])
    c6 = pltpu.make_async_copy(len_hbm, len_ref, loc_sem.at[6])
    c7 = pltpu.make_async_copy(sink_hbm, sink_ref, loc_sem.at[7])
    for c in (c0, c1, c2, c3, c4, c5, c6, c7):
        c.start()

    for c in (c0, c1, c2, c3):
        c.wait()
    pl.semaphore_wait(barrier, NY - 1 + 2)

    def cell(ref, slot, c):
        return ref.at[pl.ds(pl.multiple_of(slot * (2 * R) + c * R, R), R), :]

    def up_slot(zz, j):
        return j + jnp.maximum(0, j - (NZ - zz))

    def down_slot(zz, j):
        return jnp.where(zz + j >= NZ, 2 * j + 1 - (NZ - zz), NZ + j)

    def cross(slot, tslot, c, sems, j, zt, n):
        ref, sem = ((kbuf, kr_sem), (vbuf, vr_sem))[n]
        return pltpu.make_async_remote_copy(
            src_ref=cell(ref, slot, c),
            dst_ref=cell(ref, tslot, c),
            send_sem=sems[n].at[j, c],
            recv_sem=sem.at[tslot, c],
            device_id=dev(zt, y),
            device_id_type=MESH,
        )

    def up(slot, c, j, n):
        return cross(slot, up_slot(z + 1, j + 1), c, (kus, vus), j, (z + 1) % NZ, n)

    def down(slot, c, j, n):
        zt = (z + NZ - 1) % NZ
        return cross(slot, down_slot(zt, j + 1), c, (kds, vds), j, zt, n)

    def start_up(slot, c, j, n):
        @pl.when((j < NU) & (z < NZ - 1) & (z >= j))
        def _():
            up(slot, c, j, n).start()

    def start_down(slot, c, j, n):
        @pl.when((j < ND) & ((z + j) % NZ <= KD))
        def _():
            down(slot, c, j, n).start()

    for n in range(2):
        start_up(0, g, 0, n)
        start_down(0, g, 0, n)

    yp = y + 1 - 2 * g
    to_pair = (
        pltpu.make_async_remote_copy(
            src_ref=kx, dst_ref=cell(kbuf, 0, g), send_sem=xk_sem.at[0], recv_sem=kr_sem.at[0, g],
            device_id=dev(z, yp), device_id_type=MESH,
        ),
        pltpu.make_async_remote_copy(
            src_ref=vx, dst_ref=cell(vbuf, 0, g), send_sem=xk_sem.at[1], recv_sem=vr_sem.at[0, g],
            device_id=dev(z, yp), device_id_type=MESH,
        ),
    )
    for d in to_pair:
        d.start()

    def q_copy(i):
        src = qbuf.at[y] if i == 2 else qx
        return pltpu.make_async_remote_copy(
            src_ref=src, dst_ref=qbuf.at[y], send_sem=qs_sem.at[i], recv_sem=qr_sem.at[y],
            device_id=dev(z, (y + i) % NY), device_id_type=MESH,
        )

    lane = lax.broadcasted_iota(jnp.int32, (2 * R, D), 1)
    row = lax.broadcasted_iota(jnp.int32, (2 * R, D), 0)
    plain = jnp.where(lane < 64, 1.0, 0.0).astype(jnp.bfloat16)

    def fill(i, _):
        ebuf[pl.ds(pl.multiple_of(i * 2 * R, 2 * R), 2 * R), :] = plain
        return 0

    lax.fori_loop(0, NZ, fill, 0)
    c6.wait()
    c7.wait()
    kpos = row + b * 2 * R
    hit = kpos == sink_ref[0]
    for n in range(1, 4):
        hit = hit | (kpos == sink_ref[n])
    first = jnp.where(z < NU + 1, z, NZ + 1 - z)
    ebuf[pl.ds(pl.multiple_of(first * 2 * R, 2 * R), 2 * R), :] = jnp.where(
        (lane < 64) | hit, 1.0, 0.0
    ).astype(jnp.bfloat16)

    def wait_cell(slot, c, n):
        ref, sem = ((kbuf, kr_sem), (vbuf, vr_sem))[n]
        pltpu.make_async_remote_copy(
            src_ref=cell(ref, slot, c), dst_ref=cell(ref, slot, c), send_sem=xk_sem.at[0],
            recv_sem=sem.at[slot, c], device_id=dev(z, yp), device_id_type=MESH,
        ).wait_recv()

    def wait_q(t):
        pltpu.make_async_remote_copy(
            src_ref=qx, dst_ref=qbuf.at[t], send_sem=qs_sem.at[0], recv_sem=qr_sem.at[t],
            device_id=dev(z, yp), device_id_type=MESH,
        ).wait_recv()

    c4.wait()
    c5.wait()
    for i in (1, 3, 2):
        q_copy(i).start()

    for n in range(2):
        wait_cell(0, 1 - g, n)
        start_up(0, 1 - g, 0, n)
        start_down(0, 1 - g, 0, n)

    def poll(e, _):
        j = e // 2 + 1
        c = (g + e) % 2

        @pl.when((e > 0) & (e < NU))
        def _():
            pl.semaphore_wait(hello.at[e - 1], 2)

        @pl.when(e < NU - 1)
        def _():
            for zz in beside:
                pl.semaphore_signal(hello.at[e], inc=1, device_id=dev(zz, y), device_id_type=MESH)

        @pl.when((j <= NU) & (z >= j))
        def _():
            slot = up_slot(z, j)
            for n in range(2):
                wait_cell(slot, c, n)
                start_up(slot, c, j, n)

        @pl.when((j <= ND) & ((z + j) % NZ <= KD))
        def _():
            slot = down_slot(z, j)
            for n in range(2):
                wait_cell(slot, c, n)
                start_down(slot, c, j, n)

        return 0

    def scores(t, h, k):
        return lax.dot_general(
            qbuf[t, :, h * D : (h + 1) * D], k, (((1,), (1,)), ((), ())), preferred_element_type=jnp.float32
        )

    def weigh(sc, mn):
        mc = mn * LC
        cols = [jnp.exp2(sc[:, n * D : (n + 1) * D] * LC - mc) for n in range(sc.shape[1] // D)]
        return jnp.concatenate(cols, axis=1).astype(jnp.bfloat16)

    def mix(p, ve):
        return lax.dot_general(p, ve, (((1,), (0,)), ((), ())), preferred_element_type=jnp.float32)

    qi = lax.broadcasted_iota(jnp.int32, (R, 2 * R), 0)
    ki = lax.broadcasted_iota(jnp.int32, (R, 2 * R), 1)

    def attend_own(t):
        k = kbuf[0 : 2 * R, :]
        ve = jnp.concatenate([vbuf[0 : 2 * R, :], ebuf[0 : 2 * R, :]], axis=1)
        ok = ki + b * 2 * R <= qi + t * R
        sc = [jnp.where(ok, scores(t, h, k), LOW) for h in range(HG)]
        for h in range(HG):
            mn = jnp.broadcast_to(jnp.max(sc[h], axis=1, keepdims=True), (R, D))
            m_ref[t, h] = mn
            acc_ref[t, h] = mix(weigh(sc[h], mn), ve)

    def attend(t, base, n):
        rows = pl.ds(pl.multiple_of(base, 2 * R), n * 2 * R)
        k = kbuf[rows, :]
        ve = jnp.concatenate([vbuf[rows, :], ebuf[rows, :]], axis=1)
        sc = [scores(t, h, k) for h in range(HG)]
        for h in range(HG):
            mo = m_ref[t, h]
            mn = jnp.maximum(mo, jnp.max(sc[h], axis=1, keepdims=True))
            al = jnp.exp2((mo - mn) * LC)
            pv = mix(weigh(sc[h], mn), ve)
            acc_ref[t, h] = acc_ref[t, h] * jnp.concatenate([al, al], axis=1) + pv
            m_ref[t, h] = mn

    def have(st):
        j = jnp.where(st < 4, 2 * st, st + 3)
        ups = jnp.minimum(jnp.minimum(j, NU), z)
        return ups + jnp.maximum(0, jnp.minimum(j, ND) - (NZ - z) + 1)

    def item(it, e):
        k = it % 3
        st = jnp.where(it < 6, it // 3, jnp.where(it < 8, it - 6, it // 4))
        gi = jnp.where(it < 6, k + k // 2, jnp.where(it < 8, 2, gray(NY - 1 - it % 4)))
        t = (y + gi) % NY

        @pl.when(st == 0)
        def _():
            @pl.when(gi > 0)
            def _():
                wait_q(t)

            attend_own(t)

        before = have(st - 1)
        count = have(st) - before
        for n in range(1, 5):

            @pl.when((st > 0) & (count == n))
            def _():
                attend(t, (before + 1) * 2 * R, n)

        two = (it == 0) | (it == 5) | (it == 7) | (it == 11)
        one = (it == 1) | (it == 2) | (it == 9) | (it == 10)
        one = one | (it == 14) | (it == 15) | (it == 18) | (it == 19)
        polls = jnp.where(two, 2, jnp.where(one, 1, 0))
        lax.fori_loop(e, e + polls, poll, 0)
        return e + polls

    lax.fori_loop(0, 24, item, 0)

    lane1 = lax.broadcasted_iota(jnp.int32, (R, D), 1)

    def stats(t, _):
        x, m = jnp.ones((R, D), jnp.float32), jnp.zeros((R, D), jnp.float32)
        for h in range(HG):
            x = jnp.where((lane1 == h) | (lane1 == 64 + h), acc_ref[t, h, :, D : 2 * D], x)
            m = jnp.where(lane1 == h, m_ref[t, h], m)
        frac = x / pltpu.roll(x, 64, 1)
        xs_ref[...] = jnp.where(lane1 < 64, m * SCALE + jnp.log(x), frac).T
        xrecv[y, t, 0:8] = xs_ref[0:8, :]
        xrecv[y, t, 8:16] = xs_ref[64:72, :]
        return 0

    lax.fori_loop(0, NY, stats, 0)

    def tell(i):
        return pltpu.make_async_remote_copy(
            src_ref=xrecv.at[y], dst_ref=xrecv.at[y], send_sem=ss_sem.at[i], recv_sem=sr_sem.at[y],
            device_id=dev(z, (y + i) % NY), device_id_type=MESH,
        )

    def back(i):
        return pltpu.make_async_remote_copy(
            src_ref=osend.at[i], dst_ref=orecv.at[y], send_sem=os_sem.at[i], recv_sem=or_sem.at[y],
            device_id=dev(z, (y + i) % NY), device_id_type=MESH,
        )

    for i in (2, 1, 3):
        tell(i).start()

    def outputs(i, ref, at):
        t = (y + i) % NY
        for h in range(HG):
            inv = 1.0 / jnp.broadcast_to(acc_ref[t, h, :, D : D + 1], (R, D))
            ref[at, :, h * D : (h + 1) * D] = (acc_ref[t, h, :, 0:D] * inv).astype(jnp.bfloat16)

    for i in (2, 3, 1):
        outputs(i, osend, i)
    for i in (2, 3, 1):
        back(i).start()
    outputs(0, orecv, y)

    for i in range(1, NY):
        yy = (y + i) % NY
        pltpu.make_async_remote_copy(
            src_ref=xrecv.at[y], dst_ref=xrecv.at[yy], send_sem=ss_sem.at[0], recv_sem=sr_sem.at[yy],
            device_id=dev(z, yp), device_id_type=MESH,
        ).wait_recv()

    def join(gg, t):
        xa, xb = xrecv[gg, t], xrecv[2 + gg, t]
        la, lb = xa[0:8], xb[0:8]
        top = jnp.maximum(la, lb)
        ea, eb = jnp.exp(la - top), jnp.exp(lb - top)
        tot = ea + eb
        wa, wb = ea / tot, eb / tot
        pos = (z * NY + t) * R + lax.broadcasted_iota(jnp.int32, (8, D), 1)
        live = pos < len_ref[0]
        lse = jnp.where(live, top + jnp.log(tot), 0.0)
        mass = jnp.where(live, wa * xa[8:16] + wb * xb[8:16], 0.0)
        return lse, mass, jnp.where(live, wa, 0.0), jnp.where(live, wb, 0.0)

    pk_ref[...] = jnp.zeros_like(pk_ref)
    for gg in range(2):
        lse, mass = jnp.zeros((8, D), jnp.float32), jnp.zeros((8, D), jnp.float32)
        for t in range(NY):
            more = join(gg, t)
            lse, mass = lse + more[0], mass + more[1]
        pk_ref[gg * HG : (gg + 1) * HG, :] = lse[0:HG]
        pk_ref[16 + gg * HG : 16 + (gg + 1) * HG, :] = mass[0:HG]
        lse, mass, wa, wb = join(gg, y)
        lse_ref[gg * HG : (gg + 1) * HG, :] = lse[0:HG]
        mass_ref[gg * HG : (gg + 1) * HG, :] = mass[0:HG]
        pk_ref[32 + 16 * gg : 40 + 16 * gg, :] = wa
        pk_ref[40 + 16 * gg : 48 + 16 * gg, :] = wb
    xs_ref[...] = pk_ref[...].T
    zsum[z] = jnp.broadcast_to(jnp.sum(xs_ref[...], axis=0, keepdims=True), (8, D))

    def sum_z(i):
        return pltpu.make_async_remote_copy(
            src_ref=zsum.at[z], dst_ref=zsum.at[z], send_sem=zs_sem.at[i], recv_sem=zr_sem.at[z],
            device_id=dev((z + i) % NZ, y), device_id_type=MESH,
        )

    def sum_z_start(i, _):
        sum_z(i).start()
        return 0

    lax.fori_loop(1, NZ, sum_z_start, 0)

    for i in range(1, NY):
        yy = (y + i) % NY
        pltpu.make_async_remote_copy(
            src_ref=osend.at[0], dst_ref=orecv.at[yy], send_sem=os_sem.at[0], recv_sem=or_sem.at[yy],
            device_id=dev(z, yp), device_id_type=MESH,
        ).wait_recv()
    for gg in range(2):
        for h in range(HG):
            at = 32 + 16 * gg + h
            cols = slice(h * D, (h + 1) * D)
            o = xs_ref[:, at : at + 1] * orecv[gg, :, cols].astype(jnp.float32)
            o = o + xs_ref[:, at + 8 : at + 9] * orecv[2 + gg, :, cols].astype(jnp.float32)
            obuf[:, gg * CW + h * D : gg * CW + (h + 1) * D] = o.astype(jnp.bfloat16)
    places = (
        (obuf, out_hbm), (lse_ref, lse_hbm), (mass_ref, mass_hbm), (hl_ref, hl_hbm), (hs_ref, hs_hbm)
    )
    home = [pltpu.make_async_copy(a, o, loc_sem.at[n]) for n, (a, o) in enumerate(places)]
    for d in home[0:3]:
        d.start()

    def sum_z_wait(i, _):
        zz = (z + i) % NZ
        pltpu.make_async_remote_copy(
            src_ref=zsum.at[z], dst_ref=zsum.at[zz], send_sem=zs_sem.at[0], recv_sem=zr_sem.at[zz],
            device_id=dev(z, yp), device_id_type=MESH,
        ).wait_recv()
        return 0

    lax.fori_loop(1, NZ, sum_z_wait, 0)
    total = zsum[0]
    for i in range(1, NZ):
        total = total + zsum[i]
    mean = total[0:1, :] / len_ref[0].astype(jnp.float32)
    hl_ref[...] = mean[:, 0 : 2 * HG]
    hs_ref[...] = mean[:, 16 : 16 + 2 * HG]

    for d in home[3:5]:
        d.start()

    for c in range(2):
        for j in range(NU):

            @pl.when((z < NZ - 1) & (z >= j))
            def _():
                for n in range(2):
                    up(0, c, j, n).wait_send()

        for j in range(ND):

            @pl.when((z + j) % NZ <= KD)
            def _():
                for n in range(2):
                    down(0, c, j, n).wait_send()

    for d in to_pair:
        d.wait_send()
    for i in (1, 3, 2):
        q_copy(i).wait_send()
        tell(i).wait_send()
        back(i).wait_send()

    def sum_z_sent(i, _):
        sum_z(i).wait_send()
        return 0

    lax.fori_loop(1, NZ, sum_z_sent, 0)
    for d in home:
        d.wait()


def hand_on(*refs):
    n = (len(refs) - 2) // 3
    ins, outs, held = refs[:n], refs[n : 2 * n], refs[2 * n : 3 * n]
    come, go = refs[3 * n :]
    for i in range(n):
        pltpu.make_async_copy(ins[i], held[i], come.at[i]).start()
    for i in range(n):
        pltpu.make_async_copy(ins[i], held[i], come.at[i]).wait()
        pltpu.make_async_copy(held[i], outs[i], go.at[i]).start()
    for i in range(n):
        pltpu.make_async_copy(held[i], outs[i], go.at[i]).wait()


def body(queries, keys, values, doc_length, sink_pos):
    NZ = lax.axis_size("seq") // NY
    NU = NZ // 2
    cells = NZ + NU
    f32, bf16 = jnp.float32, jnp.bfloat16
    vm, dma = pltpu.VMEM, pltpu.SemaphoreType.DMA
    results = (
        jax.ShapeDtypeStruct((R, 2 * CW), bf16),
        jax.ShapeDtypeStruct((2 * HG, R), f32),
        jax.ShapeDtypeStruct((2 * HG, R), f32),
        jax.ShapeDtypeStruct((1, 2 * HG), f32),
        jax.ShapeDtypeStruct((1, 2 * HG), f32),
    )
    parts = pl.pallas_call(
        functools.partial(kernel, NZ),
        out_shape=results,
        in_specs=[
            pl.BlockSpec(memory_space=pl.ANY),
            pl.BlockSpec(memory_space=pl.ANY),
            pl.BlockSpec(memory_space=pl.ANY),
            pl.BlockSpec(memory_space=pl.ANY),
            pl.BlockSpec(memory_space=pl.ANY),
        ],
        out_specs=(pl.BlockSpec(memory_space=pl.ANY),) * 5,
        scratch_shapes=[
            pltpu.SMEM((1,), jnp.int32),
            pltpu.SMEM((4,), jnp.int32),
            vm((2 * HG, R), f32),
            vm((2 * HG, R), f32),
            vm((1, 2 * HG), f32),
            vm((1, 2 * HG), f32),
            vm((NY, R, CW), bf16),
            vm((R, CW), bf16),
            vm((cells * 2 * R, D), bf16),
            vm((cells * 2 * R, D), bf16),
            vm((R, D), bf16),
            vm((R, D), bf16),
            vm((NZ * 2 * R, D), bf16),
            vm((NY, HG, R, D), f32),
            vm((NY, HG, R, 2 * D), f32),
            vm((NY, R, CW), bf16),
            vm((NY, R, CW), bf16),
            vm((R, 2 * CW), bf16),
            vm((NY, NY, 16, R), f32),
            vm((D, R), f32),
            vm((D, R), f32),
            vm((NZ, 8, D), f32),
            dma((8,)),
            dma((NY,)),
            dma((NY,)),
            dma((2,)),
            dma((cells, 2)),
            dma((cells, 2)),
            dma((NU, 2)),
            dma((NU, 2)),
            dma((NU, 2)),
            dma((NU, 2)),
            dma((NY,)),
            dma((NY,)),
            dma((NY,)),
            dma((NY,)),
            dma((NZ,)),
            dma((NZ,)),
            pltpu.SemaphoreType.REGULAR((NU - 1,)),
        ],
        compiler_params=pltpu.CompilerParams(
            collective_id=0, has_side_effects=True, vmem_limit_bytes=56 * 2**20
        ),
    )(doc_length, sink_pos, queries, keys, values)
    out, lse, mass, hl, hs = pl.pallas_call(
        hand_on,
        out_shape=results,
        in_specs=[pl.BlockSpec(memory_space=pl.ANY)] * 5,
        out_specs=(pl.BlockSpec(memory_space=pl.ANY),) * 5,
        scratch_shapes=[vm(r.shape, r.dtype) for r in results] + [dma((5,)), dma((5,))],
    )(*parts)
    return out, lse, mass, hl.reshape(2 * HG), hs.reshape(2 * HG)


def solution(mesh):
    rows = P(("doc", "seq"), None)
    return jax.shard_map(
        body,
        mesh=mesh,
        in_specs=(rows, rows, rows, P("doc"), P("doc")),
        out_specs=(rows, P(None, ("doc", "seq")), P(None, ("doc", "seq")), P("doc"), P("doc")),
        check_vma=False,
    )
```

```python
import functools

import jax
import jax.numpy as jnp
from jax import lax
from jax.experimental import pallas as pl
from jax.experimental.pallas import tpu as pltpu
from jax.sharding import PartitionSpec as P

MESH = pl.DeviceIdType.MESH
D = 128
R = 128
NY = 4
HG = 7
CW = HG * D
SCALE = D**-0.5
LC = SCALE * 1.4426950408889634
LOW = -(2.0**60)


PLAN = (
    (0, 0, 0, 2),
    (0, 0, 1, 0),
    (1, 0, 0, 0),
    (1, 0, 1, 1),
    (3, 0, 0, 1),
    (3, 0, 2, 0),
    (0, 1, 2, 1),
    (1, 1, 2, 1),
    (2, 0, 0, 0),
    (2, 0, 2, 1),
    (0, 2, 3, 1),
    (1, 2, 4, 0),
    (2, 2, 4, 1),
    (3, 2, 4, 1),
    (0, 3, 5, 1),
    (1, 4, 5, 1),
    (2, 4, 6, 0),
    (3, 4, 6, 1),
    (0, 5, 6, 1),
    (1, 5, 7, 0),
    (0, 6, 7, 2),
    (2, 6, 8, 0),
    (3, 6, 8, 0),
    (1, 7, 8, 0),
    (0, 7, 8, 0),
)
assert sum(row[3] for row in PLAN) == 16


def pick(i, table):
    at = jnp.int32(table[0])
    for n in range(1, len(table)):
        if table[n] != table[n - 1]:
            at = at + jnp.where(i >= n, table[n] - table[n - 1], 0)
    return at


def kernel(
    NZ,
    len_hbm,
    sink_hbm,
    q_hbm,
    k_hbm,
    v_hbm,
    out_hbm,
    lse_hbm,
    mass_hbm,
    hl_hbm,
    hs_hbm,
    len_ref,
    sink_ref,
    lse_ref,
    mass_ref,
    hl_ref,
    hs_ref,
    qbuf,
    qx,
    kbuf,
    vbuf,
    kx,
    vx,
    ebuf,
    m_ref,
    acc_ref,
    osend,
    orecv,
    obuf,
    xrecv,
    xs_ref,
    pk_ref,
    zsum,
    loc_sem,
    qs_sem,
    qr_sem,
    xk_sem,
    kr_sem,
    vr_sem,
    us_sem,
    ds_sem,
    os_sem,
    or_sem,
    ss_sem,
    sr_sem,
    zs_sem,
    zr_sem,
    hello,
):
    NU = NZ // 2
    ND = NU - 1
    KD = NU - 2
    NST = NU // 2
    s = lax.axis_index("seq")
    z = s // NY
    y = s % NY
    g = y % 2
    b = y // 2

    def dev(zz, yy):
        return {"seq": zz * NY + yy}

    def lanes(ref, start, size):
        return ref.at[:, pl.ds(pl.multiple_of(start, 128), size)]

    barrier = pltpu.get_barrier_semaphore()

    beside = ((z + 1) % NZ, (z + NZ - 1) % NZ)
    for zz in beside:
        pl.semaphore_signal(barrier, inc=1, device_id=dev(zz, y), device_id_type=MESH)
    for i in range(1, NY):
        pl.semaphore_signal(barrier, inc=1, device_id=dev(z, (y + i) % NY), device_id_type=MESH)

    c0 = pltpu.make_async_copy(lanes(k_hbm, g * D, D), kbuf.at[pl.ds(pl.multiple_of(g * R, R), R), :], loc_sem.at[0])
    c1 = pltpu.make_async_copy(lanes(v_hbm, g * D, D), vbuf.at[pl.ds(pl.multiple_of(g * R, R), R), :], loc_sem.at[1])
    c2 = pltpu.make_async_copy(lanes(k_hbm, (1 - g) * D, D), kx, loc_sem.at[2])
    c3 = pltpu.make_async_copy(lanes(v_hbm, (1 - g) * D, D), vx, loc_sem.at[3])
    c4 = pltpu.make_async_copy(lanes(q_hbm, (1 - g) * CW, CW), qx, loc_sem.at[4])
    c5 = pltpu.make_async_copy(lanes(q_hbm, g * CW, CW), qbuf.at[y], loc_sem.at[5])
    c6 = pltpu.make_async_copy(len_hbm, len_ref, loc_sem.at[6])
    c7 = pltpu.make_async_copy(sink_hbm, sink_ref, loc_sem.at[7])
    for c in (c0, c1, c2, c3, c4, c5, c6, c7):
        c.start()

    for c in (c0, c1, c2, c3):
        c.wait()
    pl.semaphore_wait(barrier, NY - 1 + 2)

    def cell(ref, slot, c):
        return ref.at[pl.ds(pl.multiple_of(slot * (2 * R) + c * R, R), R), :]

    def up_slot(zz, j):
        return j + jnp.maximum(0, j - (NZ - zz))

    def down_slot(zz, j):
        return jnp.where(zz + j >= NZ, 2 * j + 1 - (NZ - zz), NZ + j)

    def cross(slot, tslot, c, sent, j, zt, n):
        ref, sem = ((kbuf, kr_sem), (vbuf, vr_sem))[n]
        return pltpu.make_async_remote_copy(
            src_ref=cell(ref, slot, c),
            dst_ref=cell(ref, tslot, c),
            send_sem=sent.at[j],
            recv_sem=sem.at[tslot, c],
            device_id=dev(zt, y),
            device_id_type=MESH,
        )

    def up(slot, c, j, n):
        return cross(slot, up_slot(z + 1, j + 1), c, us_sem, j, (z + 1) % NZ, n)

    def down(slot, c, j, n):
        zt = (z + NZ - 1) % NZ
        return cross(slot, down_slot(zt, j + 1), c, ds_sem, j, zt, n)

    def start_up(slot, c, j, n):
        @pl.when((j < NU) & (z < NZ - 1) & (z >= j))
        def _():
            up(slot, c, j, n).start()

    def start_down(slot, c, j, n):
        @pl.when((j < ND) & ((z + j) % NZ <= KD))
        def _():
            down(slot, c, j, n).start()

    for n in range(2):
        start_up(0, g, 0, n)
        start_down(0, g, 0, n)

    yp = y + 1 - 2 * g
    to_pair = (
        pltpu.make_async_remote_copy(
            src_ref=kx, dst_ref=cell(kbuf, 0, g), send_sem=xk_sem, recv_sem=kr_sem.at[0, g],
            device_id=dev(z, yp), device_id_type=MESH,
        ),
        pltpu.make_async_remote_copy(
            src_ref=vx, dst_ref=cell(vbuf, 0, g), send_sem=xk_sem, recv_sem=vr_sem.at[0, g],
            device_id=dev(z, yp), device_id_type=MESH,
        ),
    )
    for d in to_pair:
        d.start()

    def q_copy(i):
        src = qbuf.at[y] if i == 2 else qx
        return pltpu.make_async_remote_copy(
            src_ref=src, dst_ref=qbuf.at[y], send_sem=qs_sem, recv_sem=qr_sem.at[y],
            device_id=dev(z, (y + i) % NY), device_id_type=MESH,
        )

    lane = lax.broadcasted_iota(jnp.int32, (2 * R, D), 1)
    row = lax.broadcasted_iota(jnp.int32, (2 * R, D), 0)
    plain = jnp.where(lane < 64, 1.0, 0.0).astype(jnp.bfloat16)

    def fill(i, _):
        ebuf[pl.ds(pl.multiple_of(i * 2 * R, 2 * R), 2 * R), :] = plain
        return 0

    lax.fori_loop(0, NZ, fill, 0)
    c6.wait()
    c7.wait()
    kpos = row + b * 2 * R
    hit = kpos == sink_ref[0]
    for n in range(1, 4):
        hit = hit | (kpos == sink_ref[n])
    first = jnp.where(z < NU + 1, z, NZ + 1 - z)
    ebuf[pl.ds(pl.multiple_of(first * 2 * R, 2 * R), 2 * R), :] = jnp.where(
        (lane < 64) | hit, 1.0, 0.0
    ).astype(jnp.bfloat16)

    def wait_cell(slot, c, n):
        ref, sem = ((kbuf, kr_sem), (vbuf, vr_sem))[n]
        pltpu.make_async_remote_copy(
            src_ref=cell(ref, slot, c), dst_ref=cell(ref, slot, c), send_sem=xk_sem,
            recv_sem=sem.at[slot, c], device_id=dev(z, yp), device_id_type=MESH,
        ).wait_recv()

    def wait_q(t):
        pltpu.make_async_remote_copy(
            src_ref=qx, dst_ref=qbuf.at[t], send_sem=qs_sem, recv_sem=qr_sem.at[t],
            device_id=dev(z, yp), device_id_type=MESH,
        ).wait_recv()

    c4.wait()
    c5.wait()
    for i in (1, 3, 2):
        q_copy(i).start()

    for n in range(2):
        wait_cell(0, 1 - g, n)
        start_up(0, 1 - g, 0, n)
        start_down(0, 1 - g, 0, n)

    def poll(e, _):
        j = e // 2 + 1
        c = (g + e) % 2

        @pl.when((e > 0) & (e < NU))
        def _():
            pl.semaphore_wait(hello.at[e - 1], 2)

        @pl.when(e < NU - 1)
        def _():
            for zz in beside:
                pl.semaphore_signal(hello.at[e], inc=1, device_id=dev(zz, y), device_id_type=MESH)

        @pl.when((j <= NU) & (z >= j))
        def _():
            slot = up_slot(z, j)
            for n in range(2):
                wait_cell(slot, c, n)
                start_up(slot, c, j, n)

        @pl.when((j <= ND) & ((z + j) % NZ <= KD))
        def _():
            slot = down_slot(z, j)
            for n in range(2):
                wait_cell(slot, c, n)
                start_down(slot, c, j, n)

        return 0

    def scores(t, h, k):
        return lax.dot_general(
            qbuf[t, :, h * D : (h + 1) * D], k, (((1,), (1,)), ((), ())), preferred_element_type=jnp.float32
        )

    def weigh(sc, mn):
        mc = mn * LC
        cols = [jnp.exp2(sc[:, n * D : (n + 1) * D] * LC - mc) for n in range(sc.shape[1] // D)]
        return jnp.concatenate(cols, axis=1).astype(jnp.bfloat16)

    def mix(p, ve):
        return lax.dot_general(p, ve, (((1,), (0,)), ((), ())), preferred_element_type=jnp.float32)

    qi = lax.broadcasted_iota(jnp.int32, (R, 2 * R), 0)
    ki = lax.broadcasted_iota(jnp.int32, (R, 2 * R), 1)

    def attend_own(t):
        k = kbuf[0 : 2 * R, :]
        ve = jnp.concatenate([vbuf[0 : 2 * R, :], ebuf[0 : 2 * R, :]], axis=1)
        ok = ki + b * 2 * R <= qi + t * R
        sc = [jnp.where(ok, scores(t, h, k), LOW) for h in range(HG)]
        for h in range(HG):
            mn = jnp.broadcast_to(jnp.max(sc[h], axis=1, keepdims=True), (R, D))
            m_ref[t, h] = mn
            acc_ref[t, h] = mix(weigh(sc[h], mn), ve)

    def attend(t, base, n):
        rows = pl.ds(pl.multiple_of(base, 2 * R), n * 2 * R)
        k = kbuf[rows, :]
        ve = jnp.concatenate([vbuf[rows, :], ebuf[rows, :]], axis=1)
        sc = [scores(t, h, k) for h in range(HG)]
        for h in range(HG):
            mo = m_ref[t, h]
            mn = jnp.maximum(mo, jnp.max(sc[h], axis=1, keepdims=True))
            al = jnp.exp2((mo - mn) * LC)
            pv = mix(weigh(sc[h], mn), ve)
            acc_ref[t, h] = acc_ref[t, h] * jnp.concatenate([al, al], axis=1) + pv
            m_ref[t, h] = mn

    def have(j):
        ups = jnp.minimum(jnp.minimum(j, NU), z)
        return ups + jnp.maximum(0, jnp.minimum(j, ND) - (NZ - z) + 1)

    def item(it, e):
        row = pick(it, [a + 4 * (p + 4 * (j0 + 16 * j1)) for a, j0, j1, p in PLAN])
        gi, polls, j0, j1 = row % 4, row // 4 % 4, row // 16 % 16, row // 256
        t = (y + gi) % NY

        @pl.when(j1 == 0)
        def _():
            @pl.when(gi > 0)
            def _():
                wait_q(t)

            attend_own(t)

        before = have(j0)
        count = have(j1) - before
        for n in range(1, 5):

            @pl.when((j1 > 0) & (count == n))
            def _():
                attend(t, (before + 1) * 2 * R, n)

        lax.fori_loop(e, e + polls, poll, 0)
        return e + polls

    lax.fori_loop(0, len(PLAN), item, 0)

    lane1 = lax.broadcasted_iota(jnp.int32, (R, D), 1)

    def stats(t, _):
        x, m = jnp.ones((R, D), jnp.float32), jnp.zeros((R, D), jnp.float32)
        for h in range(HG):
            x = jnp.where((lane1 == h) | (lane1 == 64 + h), acc_ref[t, h, :, D : 2 * D], x)
            m = jnp.where(lane1 == h, m_ref[t, h], m)
        frac = x / pltpu.roll(x, 64, 1)
        xs_ref[...] = jnp.where(lane1 < 64, m * SCALE + jnp.log(x), frac).T
        xrecv[y, t, 0:8] = xs_ref[0:8, :]
        xrecv[y, t, 8:16] = xs_ref[64:72, :]
        return 0

    lax.fori_loop(0, NY, stats, 0)

    def tell(i):
        return pltpu.make_async_remote_copy(
            src_ref=xrecv.at[y], dst_ref=xrecv.at[y], send_sem=ss_sem, recv_sem=sr_sem,
            device_id=dev(z, (y + i) % NY), device_id_type=MESH,
        )

    def back(i):
        return pltpu.make_async_remote_copy(
            src_ref=osend.at[i], dst_ref=orecv.at[y], send_sem=os_sem, recv_sem=or_sem,
            device_id=dev(z, (y + i) % NY), device_id_type=MESH,
        )

    for i in (2, 1, 3):
        tell(i).start()

    def outputs(i, ref, at):
        t = (y + i) % NY
        for h in range(HG):
            inv = 1.0 / jnp.broadcast_to(acc_ref[t, h, :, D : D + 1], (R, D))
            ref[at, :, h * D : (h + 1) * D] = (acc_ref[t, h, :, 0:D] * inv).astype(jnp.bfloat16)

    for i in (2, 3, 1):
        outputs(i, osend, i)
    for i in (2, 3, 1):
        back(i).start()
    outputs(0, orecv, y)

    def landed(ref, sem):
        pltpu.make_async_remote_copy(
            src_ref=ref, dst_ref=ref, send_sem=xk_sem, recv_sem=sem, device_id=dev(z, yp), device_id_type=MESH
        ).wait_recv()

    landed(xrecv.at[0 : NY - 1], sr_sem)

    def join(gg, t):
        xa, xb = xrecv[gg, t], xrecv[2 + gg, t]
        la, lb = xa[0:8], xb[0:8]
        top = jnp.maximum(la, lb)
        ea, eb = jnp.exp(la - top), jnp.exp(lb - top)
        tot = ea + eb
        wa, wb = ea / tot, eb / tot
        pos = (z * NY + t) * R + lax.broadcasted_iota(jnp.int32, (8, D), 1)
        live = pos < len_ref[0]
        lse = jnp.where(live, top + jnp.log(tot), 0.0)
        mass = jnp.where(live, wa * xa[8:16] + wb * xb[8:16], 0.0)
        return lse, mass, jnp.where(live, wa, 0.0), jnp.where(live, wb, 0.0)

    pk_ref[...] = jnp.zeros_like(pk_ref)
    for gg in range(2):
        lse, mass = jnp.zeros((8, D), jnp.float32), jnp.zeros((8, D), jnp.float32)
        for t in range(NY):
            more = join(gg, t)
            lse, mass = lse + more[0], mass + more[1]
        pk_ref[gg * HG : (gg + 1) * HG, :] = lse[0:HG]
        pk_ref[16 + gg * HG : 16 + (gg + 1) * HG, :] = mass[0:HG]
        lse, mass, wa, wb = join(gg, y)
        lse_ref[gg * HG : (gg + 1) * HG, :] = lse[0:HG]
        mass_ref[gg * HG : (gg + 1) * HG, :] = mass[0:HG]
        pk_ref[32 + 16 * gg : 40 + 16 * gg, :] = wa
        pk_ref[40 + 16 * gg : 48 + 16 * gg, :] = wb
    xs_ref[...] = pk_ref[...].T
    zsum[z] = jnp.broadcast_to(jnp.sum(xs_ref[...], axis=0, keepdims=True), (8, D))

    def sum_z(i):
        return pltpu.make_async_remote_copy(
            src_ref=zsum.at[z], dst_ref=zsum.at[z], send_sem=zs_sem, recv_sem=zr_sem,
            device_id=dev((z + i) % NZ, y), device_id_type=MESH,
        )

    def sum_z_start(i, _):
        sum_z(i).start()
        return 0

    lax.fori_loop(1, NZ, sum_z_start, 0)

    landed(orecv.at[0 : NY - 1], or_sem)
    for gg in range(2):
        for h in range(HG):
            at = 32 + 16 * gg + h
            cols = slice(h * D, (h + 1) * D)
            o = xs_ref[:, at : at + 1] * orecv[gg, :, cols].astype(jnp.float32)
            o = o + xs_ref[:, at + 8 : at + 9] * orecv[2 + gg, :, cols].astype(jnp.float32)
            obuf[:, gg * CW + h * D : gg * CW + (h + 1) * D] = o.astype(jnp.bfloat16)
    places = (
        (obuf, out_hbm), (lse_ref, lse_hbm), (mass_ref, mass_hbm), (hl_ref, hl_hbm), (hs_ref, hs_hbm)
    )
    home = [pltpu.make_async_copy(a, o, loc_sem.at[n]) for n, (a, o) in enumerate(places)]
    for d in home[0:3]:
        d.start()

    landed(zsum.at[0 : NZ - 1], zr_sem)
    total = zsum[0]
    for i in range(1, NZ):
        total = total + zsum[i]
    mean = total[0:1, :] / len_ref[0].astype(jnp.float32)
    hl_ref[...] = mean[:, 0 : 2 * HG]
    hs_ref[...] = mean[:, 16 : 16 + 2 * HG]

    for d in home[3:5]:
        d.start()

    def left(ref, sem):
        pltpu.make_async_remote_copy(
            src_ref=ref, dst_ref=ref, send_sem=sem, recv_sem=xk_sem, device_id=dev(z, yp), device_id_type=MESH
        ).wait_send()

    for j in range(NU):

        @pl.when((z < NZ - 1) & (z >= j))
        def _():
            left(kbuf.at[0 : 4 * R, :], us_sem.at[j])

    for j in range(ND):

        @pl.when((z + j) % NZ <= KD)
        def _():
            left(kbuf.at[0 : 4 * R, :], ds_sem.at[j])

    left(kbuf.at[0 : 2 * R, :], xk_sem)
    left(qbuf.at[0 : NY - 1], qs_sem)
    left(xrecv.at[0 : NY - 1], ss_sem)
    left(osend.at[0 : NY - 1], os_sem)
    left(zsum.at[0 : NZ - 1], zs_sem)
    for d in home:
        d.wait()


def hand_on(*refs):
    n = (len(refs) - 2) // 3
    ins, outs, held = refs[:n], refs[n : 2 * n], refs[2 * n : 3 * n]
    come, go = refs[3 * n :]
    for i in range(n):
        pltpu.make_async_copy(ins[i], held[i], come.at[i]).start()
    for i in range(n):
        pltpu.make_async_copy(ins[i], held[i], come.at[i]).wait()
        pltpu.make_async_copy(held[i], outs[i], go.at[i]).start()
    for i in range(n):
        pltpu.make_async_copy(held[i], outs[i], go.at[i]).wait()


def body(queries, keys, values, doc_length, sink_pos):
    NZ = lax.axis_size("seq") // NY
    NU = NZ // 2
    cells = NZ + NU
    f32, bf16 = jnp.float32, jnp.bfloat16
    vm, dma = pltpu.VMEM, pltpu.SemaphoreType.DMA
    results = (
        jax.ShapeDtypeStruct((R, 2 * CW), bf16),
        jax.ShapeDtypeStruct((2 * HG, R), f32),
        jax.ShapeDtypeStruct((2 * HG, R), f32),
        jax.ShapeDtypeStruct((1, 2 * HG), f32),
        jax.ShapeDtypeStruct((1, 2 * HG), f32),
    )
    parts = pl.pallas_call(
        functools.partial(kernel, NZ),
        out_shape=results,
        in_specs=[
            pl.BlockSpec(memory_space=pl.ANY),
            pl.BlockSpec(memory_space=pl.ANY),
            pl.BlockSpec(memory_space=pl.ANY),
            pl.BlockSpec(memory_space=pl.ANY),
            pl.BlockSpec(memory_space=pl.ANY),
        ],
        out_specs=(pl.BlockSpec(memory_space=pl.ANY),) * 5,
        scratch_shapes=[
            pltpu.SMEM((1,), jnp.int32),
            pltpu.SMEM((4,), jnp.int32),
            vm((2 * HG, R), f32),
            vm((2 * HG, R), f32),
            vm((1, 2 * HG), f32),
            vm((1, 2 * HG), f32),
            vm((NY, R, CW), bf16),
            vm((R, CW), bf16),
            vm((cells * 2 * R, D), bf16),
            vm((cells * 2 * R, D), bf16),
            vm((R, D), bf16),
            vm((R, D), bf16),
            vm((NZ * 2 * R, D), bf16),
            vm((NY, HG, R, D), f32),
            vm((NY, HG, R, 2 * D), f32),
            vm((NY, R, CW), bf16),
            vm((NY, R, CW), bf16),
            vm((R, 2 * CW), bf16),
            vm((NY, NY, 16, R), f32),
            vm((D, R), f32),
            vm((D, R), f32),
            vm((NZ, 8, D), f32),
            dma((8,)),
            dma,
            dma((NY,)),
            dma,
            dma((cells, 2)),
            dma((cells, 2)),
            dma((NU,)),
            dma((NU,)),
            dma,
            dma,
            dma,
            dma,
            dma,
            dma,
            pltpu.SemaphoreType.REGULAR((NU - 1,)),
        ],
        compiler_params=pltpu.CompilerParams(
            collective_id=0, has_side_effects=True, vmem_limit_bytes=56 * 2**20
        ),
    )(doc_length, sink_pos, queries, keys, values)
    out, lse, mass, hl, hs = pl.pallas_call(
        hand_on,
        out_shape=results,
        in_specs=[pl.BlockSpec(memory_space=pl.ANY)] * 5,
        out_specs=(pl.BlockSpec(memory_space=pl.ANY),) * 5,
        scratch_shapes=[vm(r.shape, r.dtype) for r in results] + [dma((5,)), dma((5,))],
    )(*parts)
    return out, lse, mass, hl.reshape(2 * HG), hs.reshape(2 * HG)


def solution(mesh):
    rows = P(("doc", "seq"), None)
    return jax.shard_map(
        body,
        mesh=mesh,
        in_specs=(rows, rows, rows, P("doc"), P("doc")),
        out_specs=(rows, P(None, ("doc", "seq")), P(None, ("doc", "seq")), P("doc"), P("doc")),
        check_vma=False,
    )
```

```python
import functools

import jax
import jax.numpy as jnp
from jax import lax
from jax.experimental import pallas as pl
from jax.experimental.pallas import tpu as pltpu
from jax.sharding import PartitionSpec as P

MESH = pl.DeviceIdType.MESH
D = 128
R = 128
NY = 4
HG = 7
CW = HG * D
SCALE = D**-0.5
LC = SCALE * 1.4426950408889634
LOW = -(2.0**60)


PLAN = (
    (0, 0, 0, 2),
    (0, 0, 1, 0),
    (1, 0, 0, 0),
    (1, 0, 1, 1),
    (3, 0, 0, 1),
    (3, 0, 2, 0),
    (0, 1, 2, 1),
    (1, 1, 2, 1),
    (2, 0, 0, 0),
    (2, 0, 2, 1),
    (0, 2, 3, 1),
    (1, 2, 4, 0),
    (2, 2, 4, 1),
    (3, 2, 4, 1),
    (0, 3, 5, 1),
    (1, 4, 5, 1),
    (2, 4, 6, 0),
    (3, 4, 6, 1),
    (0, 5, 6, 1),
    (1, 5, 7, 0),
    (0, 6, 7, 2),
    (2, 6, 8, 0),
    (3, 6, 8, 0),
    (1, 7, 8, 0),
    (0, 7, 8, 0),
)
assert sum(row[3] for row in PLAN) == 16


def pick(i, table):
    at = jnp.int32(table[0])
    for n in range(1, len(table)):
        if table[n] != table[n - 1]:
            at = at + jnp.where(i >= n, table[n] - table[n - 1], 0)
    return at


def kernel(
    NZ,
    len_hbm,
    sink_hbm,
    q_hbm,
    k_hbm,
    v_hbm,
    out_hbm,
    lse_hbm,
    mass_hbm,
    hl_hbm,
    hs_hbm,
    len_ref,
    sink_ref,
    lse_ref,
    mass_ref,
    hl_ref,
    hs_ref,
    qbuf,
    qx,
    kbuf,
    vbuf,
    kx,
    vx,
    ebuf,
    m_ref,
    acc_ref,
    osend,
    orecv,
    obuf,
    xrecv,
    xs_ref,
    pk_ref,
    zsum,
    loc_sem,
    qs_sem,
    qr_sem,
    xk_sem,
    kr_sem,
    vr_sem,
    us_sem,
    ds_sem,
    os_sem,
    or_sem,
    ss_sem,
    sr_sem,
    zs_sem,
    zr_sem,
    hello,
):
    NU = NZ // 2
    ND = NU - 1
    KD = NU - 2
    NST = NU // 2
    s = lax.axis_index("seq")
    z = s // NY
    y = s % NY
    g = y % 2
    b = y // 2

    def dev(zz, yy):
        return {"seq": zz * NY + yy}

    def lanes(ref, start, size):
        return ref.at[:, pl.ds(pl.multiple_of(start, 128), size)]

    barrier = pltpu.get_barrier_semaphore()

    beside = ((z + 1) % NZ, (z + NZ - 1) % NZ)
    for zz in beside:
        pl.semaphore_signal(barrier, inc=1, device_id=dev(zz, y), device_id_type=MESH)
    for i in range(1, NY):
        pl.semaphore_signal(barrier, inc=1, device_id=dev(z, (y + i) % NY), device_id_type=MESH)
    yp = y + 1 - 2 * g
    pl.semaphore_signal(barrier, inc=1, device_id=dev(beside[1], yp), device_id_type=MESH)

    c0 = pltpu.make_async_copy(lanes(k_hbm, g * D, D), kbuf.at[pl.ds(pl.multiple_of(g * R, R), R), :], loc_sem.at[0])
    c1 = pltpu.make_async_copy(lanes(v_hbm, g * D, D), vbuf.at[pl.ds(pl.multiple_of(g * R, R), R), :], loc_sem.at[1])
    c2 = pltpu.make_async_copy(lanes(k_hbm, (1 - g) * D, D), kx, loc_sem.at[2])
    c3 = pltpu.make_async_copy(lanes(v_hbm, (1 - g) * D, D), vx, loc_sem.at[3])
    c4 = pltpu.make_async_copy(lanes(q_hbm, (1 - g) * CW, CW), qx, loc_sem.at[4])
    c5 = pltpu.make_async_copy(lanes(q_hbm, g * CW, CW), qbuf.at[y], loc_sem.at[5])
    c6 = pltpu.make_async_copy(len_hbm, len_ref, loc_sem.at[6])
    c7 = pltpu.make_async_copy(sink_hbm, sink_ref, loc_sem.at[7])
    for c in (c0, c1, c2, c3, c4, c5, c6, c7):
        c.start()

    for c in (c0, c1, c2, c3):
        c.wait()
    pl.semaphore_wait(barrier, NY - 1 + 3)

    def cell(ref, slot, c):
        return ref.at[pl.ds(pl.multiple_of(slot * (2 * R) + c * R, R), R), :]

    def up_slot(zz, j):
        return j + jnp.maximum(0, j - (NZ - zz))

    def down_slot(zz, j):
        return jnp.where(zz + j >= NZ, 2 * j + 1 - (NZ - zz), NZ + j)

    def cross(slot, tslot, c, sent, j, zt, n):
        ref, sem = ((kbuf, kr_sem), (vbuf, vr_sem))[n]
        return pltpu.make_async_remote_copy(
            src_ref=cell(ref, slot, c),
            dst_ref=cell(ref, tslot, c),
            send_sem=sent.at[j],
            recv_sem=sem.at[tslot, c],
            device_id=dev(zt, y),
            device_id_type=MESH,
        )

    def up(slot, c, j, n):
        return cross(slot, up_slot(z + 1, j + 1), c, us_sem, j, (z + 1) % NZ, n)

    def down(slot, c, j, n):
        zt = (z + NZ - 1) % NZ
        return cross(slot, down_slot(zt, j + 1), c, ds_sem, j, zt, n)

    def start_up(slot, c, j, n):
        @pl.when((j < NU) & (z < NZ - 1) & (z >= j))
        def _():
            up(slot, c, j, n).start()

    def start_down(slot, c, j, n):
        @pl.when((j < ND) & ((z + j) % NZ <= KD))
        def _():
            down(slot, c, j, n).start()

    for n in range(2):
        start_up(0, g, 0, n)
        start_down(0, g, 0, n)

    to_pair = (
        pltpu.make_async_remote_copy(
            src_ref=kx, dst_ref=cell(kbuf, 0, g), send_sem=xk_sem, recv_sem=kr_sem.at[0, g],
            device_id=dev(z, yp), device_id_type=MESH,
        ),
        pltpu.make_async_remote_copy(
            src_ref=vx, dst_ref=cell(vbuf, 0, g), send_sem=xk_sem, recv_sem=vr_sem.at[0, g],
            device_id=dev(z, yp), device_id_type=MESH,
        ),
    )
    for d in to_pair:
        d.start()

    @pl.when(z < NZ - 1)
    def _():
        for ref, dst, sem in ((kx, kbuf, kr_sem), (vx, vbuf, vr_sem)):
            pltpu.make_async_remote_copy(
                src_ref=ref, dst_ref=cell(dst, up_slot(z + 1, 1), g), send_sem=us_sem.at[0],
                recv_sem=sem.at[up_slot(z + 1, 1), g], device_id=dev((z + 1) % NZ, yp), device_id_type=MESH,
            ).start()

    def q_copy(i):
        src = qbuf.at[y] if i == 2 else qx
        return pltpu.make_async_remote_copy(
            src_ref=src, dst_ref=qbuf.at[y], send_sem=qs_sem, recv_sem=qr_sem.at[y],
            device_id=dev(z, (y + i) % NY), device_id_type=MESH,
        )

    lane = lax.broadcasted_iota(jnp.int32, (2 * R, D), 1)
    row = lax.broadcasted_iota(jnp.int32, (2 * R, D), 0)
    plain = jnp.where(lane < 64, 1.0, 0.0).astype(jnp.bfloat16)

    def fill(i, _):
        ebuf[pl.ds(pl.multiple_of(i * 2 * R, 2 * R), 2 * R), :] = plain
        return 0

    lax.fori_loop(0, NZ, fill, 0)
    c6.wait()
    c7.wait()
    kpos = row + b * 2 * R
    hit = kpos == sink_ref[0]
    for n in range(1, 4):
        hit = hit | (kpos == sink_ref[n])
    first = jnp.where(z < NU + 1, z, NZ + 1 - z)
    ebuf[pl.ds(pl.multiple_of(first * 2 * R, 2 * R), 2 * R), :] = jnp.where(
        (lane < 64) | hit, 1.0, 0.0
    ).astype(jnp.bfloat16)

    def wait_cell(slot, c, n):
        ref, sem = ((kbuf, kr_sem), (vbuf, vr_sem))[n]
        pltpu.make_async_remote_copy(
            src_ref=cell(ref, slot, c), dst_ref=cell(ref, slot, c), send_sem=xk_sem,
            recv_sem=sem.at[slot, c], device_id=dev(z, yp), device_id_type=MESH,
        ).wait_recv()

    def wait_q(t):
        pltpu.make_async_remote_copy(
            src_ref=qx, dst_ref=qbuf.at[t], send_sem=qs_sem, recv_sem=qr_sem.at[t],
            device_id=dev(z, yp), device_id_type=MESH,
        ).wait_recv()

    c4.wait()
    c5.wait()
    for i in (1, 3, 2):
        q_copy(i).start()

    for n in range(2):
        wait_cell(0, 1 - g, n)
        start_down(0, 1 - g, 0, n)

    def poll(e, _):
        j = e // 2 + 1
        c = (g + e) % 2

        @pl.when((j <= NU) & (z >= j))
        def _():
            slot = up_slot(z, j)
            for n in range(2):
                wait_cell(slot, c, n)
                start_up(slot, c, j, n)

        @pl.when((j <= ND) & ((z + j) % NZ <= KD))
        def _():
            slot = down_slot(z, j)
            for n in range(2):
                wait_cell(slot, c, n)
                start_down(slot, c, j, n)

        r = e // 2

        @pl.when((e % 2 == 0) & (r > 0) & (r < NU))
        def _():
            pl.semaphore_wait(hello.at[r - 1], 2)

        @pl.when((e % 2 == 0) & (r < NU - 1))
        def _():
            for zz in beside:
                pl.semaphore_signal(hello.at[r], inc=1, device_id=dev(zz, y), device_id_type=MESH)

        return 0

    def scores(t, h, k):
        return lax.dot_general(
            qbuf[t, :, h * D : (h + 1) * D], k, (((1,), (1,)), ((), ())), preferred_element_type=jnp.float32
        )

    def weigh(sc, mn):
        mc = mn * LC
        cols = [jnp.exp2(sc[:, n * D : (n + 1) * D] * LC - mc) for n in range(sc.shape[1] // D)]
        return jnp.concatenate(cols, axis=1).astype(jnp.bfloat16)

    def mix(p, ve):
        return lax.dot_general(p, ve, (((1,), (0,)), ((), ())), preferred_element_type=jnp.float32)

    qi = lax.broadcasted_iota(jnp.int32, (R, 2 * R), 0)
    ki = lax.broadcasted_iota(jnp.int32, (R, 2 * R), 1)

    def attend_own(t):
        k = kbuf[0 : 2 * R, :]
        ve = jnp.concatenate([vbuf[0 : 2 * R, :], ebuf[0 : 2 * R, :]], axis=1)
        ok = ki + b * 2 * R <= qi + t * R
        sc = [jnp.where(ok, scores(t, h, k), LOW) for h in range(HG)]
        for h in range(HG):
            mn = jnp.broadcast_to(jnp.max(sc[h], axis=1, keepdims=True), (R, D))
            m_ref[t, h] = mn
            acc_ref[t, h] = mix(weigh(sc[h], mn), ve)

    def attend(t, base, n):
        rows = pl.ds(pl.multiple_of(base, 2 * R), n * 2 * R)
        k = kbuf[rows, :]
        ve = jnp.concatenate([vbuf[rows, :], ebuf[rows, :]], axis=1)
        sc = [scores(t, h, k) for h in range(HG)]
        for h in range(HG):
            mo = m_ref[t, h]
            mn = jnp.maximum(mo, jnp.max(sc[h], axis=1, keepdims=True))
            al = jnp.exp2((mo - mn) * LC)
            pv = mix(weigh(sc[h], mn), ve)
            acc_ref[t, h] = acc_ref[t, h] * jnp.concatenate([al, al], axis=1) + pv
            m_ref[t, h] = mn

    def have(j):
        ups = jnp.minimum(jnp.minimum(j, NU), z)
        return ups + jnp.maximum(0, jnp.minimum(j, ND) - (NZ - z) + 1)

    def item(it, e):
        row = pick(it, [a + 4 * (p + 4 * (j0 + 16 * j1)) for a, j0, j1, p in PLAN])
        gi, polls, j0, j1 = row % 4, row // 4 % 4, row // 16 % 16, row // 256
        gi = jnp.where((gi % 2 == 1) & (g == 0), 4 - gi, gi)
        t = (y + gi) % NY

        @pl.when(j1 == 0)
        def _():
            @pl.when(gi > 0)
            def _():
                wait_q(t)

            attend_own(t)

        before = have(j0)
        count = have(j1) - before
        for n in range(1, 5):

            @pl.when((j1 > 0) & (count == n))
            def _():
                attend(t, (before + 1) * 2 * R, n)

        lax.fori_loop(e, e + polls, poll, 0)
        return e + polls

    lax.fori_loop(0, len(PLAN), item, 0)

    lane1 = lax.broadcasted_iota(jnp.int32, (R, D), 1)

    def stats(t, _):
        x, m = jnp.ones((R, D), jnp.float32), jnp.zeros((R, D), jnp.float32)
        for h in range(HG):
            x = jnp.where((lane1 == h) | (lane1 == 64 + h), acc_ref[t, h, :, D : 2 * D], x)
            m = jnp.where(lane1 == h, m_ref[t, h], m)
        frac = x / pltpu.roll(x, 64, 1)
        xs_ref[...] = jnp.where(lane1 < 64, m * SCALE + jnp.log(x), frac).T
        xrecv[y, t, 0:8] = xs_ref[0:8, :]
        xrecv[y, t, 8:16] = xs_ref[64:72, :]
        return 0

    lax.fori_loop(0, NY, stats, 0)

    def tell(i):
        return pltpu.make_async_remote_copy(
            src_ref=xrecv.at[y], dst_ref=xrecv.at[y], send_sem=ss_sem, recv_sem=sr_sem,
            device_id=dev(z, (y + i) % NY), device_id_type=MESH,
        )

    def back(i):
        return pltpu.make_async_remote_copy(
            src_ref=osend.at[i], dst_ref=orecv.at[y], send_sem=os_sem, recv_sem=or_sem,
            device_id=dev(z, (y + i) % NY), device_id_type=MESH,
        )

    for i in (2, 1, 3):
        tell(i).start()

    def outputs(i, ref, at):
        t = (y + i) % NY
        for h in range(HG):
            inv = 1.0 / jnp.broadcast_to(acc_ref[t, h, :, D : D + 1], (R, D))
            ref[at, :, h * D : (h + 1) * D] = (acc_ref[t, h, :, 0:D] * inv).astype(jnp.bfloat16)

    for i in (2, 3, 1):
        outputs(i, osend, i)
    for i in (2, 3, 1):
        back(i).start()
    outputs(0, orecv, y)

    def landed(ref, sem):
        pltpu.make_async_remote_copy(
            src_ref=ref, dst_ref=ref, send_sem=xk_sem, recv_sem=sem, device_id=dev(z, yp), device_id_type=MESH
        ).wait_recv()

    landed(xrecv.at[0 : NY - 1], sr_sem)

    def join(gg, t):
        xa, xb = xrecv[gg, t], xrecv[2 + gg, t]
        la, lb = xa[0:8], xb[0:8]
        top = jnp.maximum(la, lb)
        ea, eb = jnp.exp(la - top), jnp.exp(lb - top)
        tot = ea + eb
        wa, wb = ea / tot, eb / tot
        pos = (z * NY + t) * R + lax.broadcasted_iota(jnp.int32, (8, D), 1)
        live = pos < len_ref[0]
        lse = jnp.where(live, top + jnp.log(tot), 0.0)
        mass = jnp.where(live, wa * xa[8:16] + wb * xb[8:16], 0.0)
        return lse, mass, jnp.where(live, wa, 0.0), jnp.where(live, wb, 0.0)

    pk_ref[...] = jnp.zeros_like(pk_ref)
    for gg in range(2):
        lse, mass = jnp.zeros((8, D), jnp.float32), jnp.zeros((8, D), jnp.float32)
        for t in range(NY):
            more = join(gg, t)
            lse, mass = lse + more[0], mass + more[1]
        pk_ref[gg * HG : (gg + 1) * HG, :] = lse[0:HG]
        pk_ref[16 + gg * HG : 16 + (gg + 1) * HG, :] = mass[0:HG]
        lse, mass, wa, wb = join(gg, y)
        lse_ref[gg * HG : (gg + 1) * HG, :] = lse[0:HG]
        mass_ref[gg * HG : (gg + 1) * HG, :] = mass[0:HG]
        pk_ref[32 + 16 * gg : 40 + 16 * gg, :] = wa
        pk_ref[40 + 16 * gg : 48 + 16 * gg, :] = wb
    xs_ref[...] = pk_ref[...].T
    zsum[z] = jnp.broadcast_to(jnp.sum(xs_ref[...], axis=0, keepdims=True), (8, D))

    def sum_z(i):
        return pltpu.make_async_remote_copy(
            src_ref=zsum.at[z], dst_ref=zsum.at[z], send_sem=zs_sem, recv_sem=zr_sem,
            device_id=dev((z + i) % NZ, y), device_id_type=MESH,
        )

    def sum_z_start(i, _):
        sum_z(i).start()
        return 0

    lax.fori_loop(1, NZ, sum_z_start, 0)

    landed(orecv.at[0 : NY - 1], or_sem)
    for gg in range(2):
        for h in range(HG):
            at = 32 + 16 * gg + h
            cols = slice(h * D, (h + 1) * D)
            o = xs_ref[:, at : at + 1] * orecv[gg, :, cols].astype(jnp.float32)
            o = o + xs_ref[:, at + 8 : at + 9] * orecv[2 + gg, :, cols].astype(jnp.float32)
            obuf[:, gg * CW + h * D : gg * CW + (h + 1) * D] = o.astype(jnp.bfloat16)
    places = (
        (obuf, out_hbm), (lse_ref, lse_hbm), (mass_ref, mass_hbm), (hl_ref, hl_hbm), (hs_ref, hs_hbm)
    )
    home = [pltpu.make_async_copy(a, o, loc_sem.at[n]) for n, (a, o) in enumerate(places)]
    for d in home[0:3]:
        d.start()

    landed(zsum.at[0 : NZ - 1], zr_sem)
    total = zsum[0]
    for i in range(1, NZ):
        total = total + zsum[i]
    mean = total[0:1, :] / len_ref[0].astype(jnp.float32)
    hl_ref[...] = mean[:, 0 : 2 * HG]
    hs_ref[...] = mean[:, 16 : 16 + 2 * HG]

    for d in home[3:5]:
        d.start()

    def left(ref, sem):
        pltpu.make_async_remote_copy(
            src_ref=ref, dst_ref=ref, send_sem=sem, recv_sem=xk_sem, device_id=dev(z, yp), device_id_type=MESH
        ).wait_send()

    for j in range(NU):

        @pl.when((z < NZ - 1) & (z >= j))
        def _():
            left(kbuf.at[0 : 4 * R, :], us_sem.at[j])

    for j in range(ND):

        @pl.when((z + j) % NZ <= KD)
        def _():
            left(kbuf.at[0 : 4 * R, :], ds_sem.at[j])

    left(kbuf.at[0 : 2 * R, :], xk_sem)
    left(qbuf.at[0 : NY - 1], qs_sem)
    left(xrecv.at[0 : NY - 1], ss_sem)
    left(osend.at[0 : NY - 1], os_sem)
    left(zsum.at[0 : NZ - 1], zs_sem)
    for d in home:
        d.wait()


def hand_on(*refs):
    n = (len(refs) - 2) // 3
    ins, outs, held = refs[:n], refs[n : 2 * n], refs[2 * n : 3 * n]
    come, go = refs[3 * n :]
    for i in range(n):
        pltpu.make_async_copy(ins[i], held[i], come.at[i]).start()
    for i in range(n):
        pltpu.make_async_copy(ins[i], held[i], come.at[i]).wait()
        pltpu.make_async_copy(held[i], outs[i], go.at[i]).start()
    for i in range(n):
        pltpu.make_async_copy(held[i], outs[i], go.at[i]).wait()


def body(queries, keys, values, doc_length, sink_pos):
    NZ = lax.axis_size("seq") // NY
    NU = NZ // 2
    cells = NZ + NU
    f32, bf16 = jnp.float32, jnp.bfloat16
    vm, dma = pltpu.VMEM, pltpu.SemaphoreType.DMA
    results = (
        jax.ShapeDtypeStruct((R, 2 * CW), bf16),
        jax.ShapeDtypeStruct((2 * HG, R), f32),
        jax.ShapeDtypeStruct((2 * HG, R), f32),
        jax.ShapeDtypeStruct((1, 2 * HG), f32),
        jax.ShapeDtypeStruct((1, 2 * HG), f32),
    )
    parts = pl.pallas_call(
        functools.partial(kernel, NZ),
        out_shape=results,
        in_specs=[
            pl.BlockSpec(memory_space=pl.ANY),
            pl.BlockSpec(memory_space=pl.ANY),
            pl.BlockSpec(memory_space=pl.ANY),
            pl.BlockSpec(memory_space=pl.ANY),
            pl.BlockSpec(memory_space=pl.ANY),
        ],
        out_specs=(pl.BlockSpec(memory_space=pl.ANY),) * 5,
        scratch_shapes=[
            pltpu.SMEM((1,), jnp.int32),
            pltpu.SMEM((4,), jnp.int32),
            vm((2 * HG, R), f32),
            vm((2 * HG, R), f32),
            vm((1, 2 * HG), f32),
            vm((1, 2 * HG), f32),
            vm((NY, R, CW), bf16),
            vm((R, CW), bf16),
            vm((cells * 2 * R, D), bf16),
            vm((cells * 2 * R, D), bf16),
            vm((R, D), bf16),
            vm((R, D), bf16),
            vm((NZ * 2 * R, D), bf16),
            vm((NY, HG, R, D), f32),
            vm((NY, HG, R, 2 * D), f32),
            vm((NY, R, CW), bf16),
            vm((NY, R, CW), bf16),
            vm((R, 2 * CW), bf16),
            vm((NY, NY, 16, R), f32),
            vm((D, R), f32),
            vm((D, R), f32),
            vm((NZ, 8, D), f32),
            dma((8,)),
            dma,
            dma((NY,)),
            dma,
            dma((cells, 2)),
            dma((cells, 2)),
            dma((NU,)),
            dma((NU,)),
            dma,
            dma,
            dma,
            dma,
            dma,
            dma,
            pltpu.SemaphoreType.REGULAR((NU - 1,)),
        ],
        compiler_params=pltpu.CompilerParams(
            collective_id=0, has_side_effects=True, vmem_limit_bytes=56 * 2**20
        ),
    )(doc_length, sink_pos, queries, keys, values)
    out, lse, mass, hl, hs = pl.pallas_call(
        hand_on,
        out_shape=results,
        in_specs=[pl.BlockSpec(memory_space=pl.ANY)] * 5,
        out_specs=(pl.BlockSpec(memory_space=pl.ANY),) * 5,
        scratch_shapes=[vm(r.shape, r.dtype) for r in results] + [dma((5,)), dma((5,))],
    )(*parts)
    return out, lse, mass, hl.reshape(2 * HG), hs.reshape(2 * HG)


def solution(mesh):
    rows = P(("doc", "seq"), None)
    return jax.shard_map(
        body,
        mesh=mesh,
        in_specs=(rows, rows, rows, P("doc"), P("doc")),
        out_specs=(rows, P(None, ("doc", "seq")), P(None, ("doc", "seq")), P("doc"), P("doc")),
        check_vma=False,
    )
```

```python
import functools

import jax
import jax.numpy as jnp
from jax import lax
from jax.experimental import pallas as pl
from jax.experimental.pallas import tpu as pltpu
from jax.sharding import PartitionSpec as P

MESH = pl.DeviceIdType.MESH
D = 128
R = 128
NY = 4
HG = 7
CW = HG * D
SCALE = D**-0.5
LC = SCALE * 1.4426950408889634
LOW = -(2.0**60)


PLAN = (
    (0, 0, 0, 2),
    (0, 0, 1, 0),
    (1, 0, 0, 0),
    (1, 0, 1, 1),
    (3, 0, 0, 1),
    (3, 0, 2, 0),
    (0, 1, 2, 1),
    (1, 1, 2, 1),
    (2, 0, 0, 0),
    (2, 0, 2, 1),
    (0, 2, 3, 1),
    (1, 2, 4, 0),
    (2, 2, 4, 1),
    (3, 2, 4, 1),
    (0, 3, 5, 1),
    (1, 4, 5, 1),
    (2, 4, 6, 0),
    (3, 4, 6, 2),
    (1, 5, 7, 0),
    (0, 5, 7, 2),
    (2, 6, 8, 0),
    (3, 6, 8, 0),
    (1, 7, 8, 0),
    (0, 7, 8, 0),
)
assert sum(row[3] for row in PLAN) == 16


def pick(i, table):
    at = jnp.int32(table[0])
    for n in range(1, len(table)):
        if table[n] != table[n - 1]:
            at = at + jnp.where(i >= n, table[n] - table[n - 1], 0)
    return at


def kernel(
    NZ,
    len_hbm,
    sink_hbm,
    q_hbm,
    k_hbm,
    v_hbm,
    out_hbm,
    lse_hbm,
    mass_hbm,
    hl_hbm,
    hs_hbm,
    len_ref,
    sink_ref,
    lse_ref,
    mass_ref,
    hl_ref,
    hs_ref,
    qbuf,
    qx,
    kbuf,
    vbuf,
    kx,
    vx,
    ebuf,
    m_ref,
    acc_ref,
    osend,
    orecv,
    obuf,
    xrecv,
    xs_ref,
    pk_ref,
    zsum,
    loc_sem,
    qs_sem,
    qr_sem,
    xk_sem,
    kr_sem,
    vr_sem,
    us_sem,
    ds_sem,
    os_sem,
    or_sem,
    ss_sem,
    sr_sem,
    zs_sem,
    zr_sem,
    hello,
):
    NU = NZ // 2
    ND = NU - 1
    KD = NU - 2
    NST = NU // 2
    s = lax.axis_index("seq")
    z = s // NY
    y = s % NY
    g = y % 2
    b = y // 2

    def dev(zz, yy):
        return {"seq": zz * NY + yy}

    def lanes(ref, start, size):
        return ref.at[:, pl.ds(pl.multiple_of(start, 128), size)]

    barrier = pltpu.get_barrier_semaphore()

    beside = ((z + 1) % NZ, (z + NZ - 1) % NZ)
    for zz in beside:
        pl.semaphore_signal(barrier, inc=1, device_id=dev(zz, y), device_id_type=MESH)
    for i in range(1, NY):
        pl.semaphore_signal(barrier, inc=1, device_id=dev(z, (y + i) % NY), device_id_type=MESH)
    yp = y + 1 - 2 * g
    pl.semaphore_signal(barrier, inc=1, device_id=dev(beside[1], yp), device_id_type=MESH)

    c0 = pltpu.make_async_copy(lanes(k_hbm, g * D, D), kbuf.at[pl.ds(pl.multiple_of(g * R, R), R), :], loc_sem.at[0])
    c1 = pltpu.make_async_copy(lanes(v_hbm, g * D, D), vbuf.at[pl.ds(pl.multiple_of(g * R, R), R), :], loc_sem.at[1])
    c2 = pltpu.make_async_copy(lanes(k_hbm, (1 - g) * D, D), kx, loc_sem.at[2])
    c3 = pltpu.make_async_copy(lanes(v_hbm, (1 - g) * D, D), vx, loc_sem.at[3])
    c4 = pltpu.make_async_copy(lanes(q_hbm, (1 - g) * CW, CW), qx, loc_sem.at[4])
    c5 = pltpu.make_async_copy(lanes(q_hbm, g * CW, CW), qbuf.at[y], loc_sem.at[5])
    c6 = pltpu.make_async_copy(len_hbm, len_ref, loc_sem.at[6])
    c7 = pltpu.make_async_copy(sink_hbm, sink_ref, loc_sem.at[7])
    for c in (c0, c1, c2, c3, c4, c5, c6, c7):
        c.start()

    for c in (c0, c1, c2, c3):
        c.wait()
    pl.semaphore_wait(barrier, NY - 1 + 3)

    def cell(ref, slot, c):
        return ref.at[pl.ds(pl.multiple_of(slot * (2 * R) + c * R, R), R), :]

    def up_slot(zz, j):
        return j + jnp.maximum(0, j - (NZ - zz))

    def down_slot(zz, j):
        return jnp.where(zz + j >= NZ, 2 * j + 1 - (NZ - zz), NZ + j)

    def cross(slot, tslot, c, sent, j, zt, n):
        ref, sem = ((kbuf, kr_sem), (vbuf, vr_sem))[n]
        return pltpu.make_async_remote_copy(
            src_ref=cell(ref, slot, c),
            dst_ref=cell(ref, tslot, c),
            send_sem=sent.at[j],
            recv_sem=sem.at[tslot, c],
            device_id=dev(zt, y),
            device_id_type=MESH,
        )

    def up(slot, c, j, n):
        return cross(slot, up_slot(z + 1, j + 1), c, us_sem, j, (z + 1) % NZ, n)

    def down(slot, c, j, n):
        zt = (z + NZ - 1) % NZ
        return cross(slot, down_slot(zt, j + 1), c, ds_sem, j, zt, n)

    def start_up(slot, c, j, n):
        @pl.when((j < NU) & (z < NZ - 1) & (z >= j))
        def _():
            up(slot, c, j, n).start()

    def start_down(slot, c, j, n):
        @pl.when((j < ND) & ((z + j) % NZ <= KD))
        def _():
            down(slot, c, j, n).start()

    for n in range(2):
        start_up(0, g, 0, n)
        start_down(0, g, 0, n)

    to_pair = (
        pltpu.make_async_remote_copy(
            src_ref=kx, dst_ref=cell(kbuf, 0, g), send_sem=xk_sem, recv_sem=kr_sem.at[0, g],
            device_id=dev(z, yp), device_id_type=MESH,
        ),
        pltpu.make_async_remote_copy(
            src_ref=vx, dst_ref=cell(vbuf, 0, g), send_sem=xk_sem, recv_sem=vr_sem.at[0, g],
            device_id=dev(z, yp), device_id_type=MESH,
        ),
    )
    for d in to_pair:
        d.start()

    @pl.when(z < NZ - 1)
    def _():
        for ref, dst, sem in ((kx, kbuf, kr_sem), (vx, vbuf, vr_sem)):
            pltpu.make_async_remote_copy(
                src_ref=ref, dst_ref=cell(dst, up_slot(z + 1, 1), g), send_sem=us_sem.at[0],
                recv_sem=sem.at[up_slot(z + 1, 1), g], device_id=dev((z + 1) % NZ, yp), device_id_type=MESH,
            ).start()

    def q_copy(i):
        src = qbuf.at[y] if i == 2 else qx
        return pltpu.make_async_remote_copy(
            src_ref=src, dst_ref=qbuf.at[y], send_sem=qs_sem, recv_sem=qr_sem.at[y],
            device_id=dev(z, (y + i) % NY), device_id_type=MESH,
        )

    lane = lax.broadcasted_iota(jnp.int32, (2 * R, D), 1)
    row = lax.broadcasted_iota(jnp.int32, (2 * R, D), 0)
    plain = jnp.where(lane < 64, 1.0, 0.0).astype(jnp.bfloat16)

    def fill(i, _):
        ebuf[pl.ds(pl.multiple_of(i * 2 * R, 2 * R), 2 * R), :] = plain
        return 0

    lax.fori_loop(0, NZ, fill, 0)
    c6.wait()
    c7.wait()
    kpos = row + b * 2 * R
    hit = kpos == sink_ref[0]
    for n in range(1, 4):
        hit = hit | (kpos == sink_ref[n])
    first = jnp.where(z < NU + 1, z, NZ + 1 - z)
    ebuf[pl.ds(pl.multiple_of(first * 2 * R, 2 * R), 2 * R), :] = jnp.where(
        (lane < 64) | hit, 1.0, 0.0
    ).astype(jnp.bfloat16)

    def wait_cell(slot, c, n):
        ref, sem = ((kbuf, kr_sem), (vbuf, vr_sem))[n]
        pltpu.make_async_remote_copy(
            src_ref=cell(ref, slot, c), dst_ref=cell(ref, slot, c), send_sem=xk_sem,
            recv_sem=sem.at[slot, c], device_id=dev(z, yp), device_id_type=MESH,
        ).wait_recv()

    def wait_q(t):
        pltpu.make_async_remote_copy(
            src_ref=qx, dst_ref=qbuf.at[t], send_sem=qs_sem, recv_sem=qr_sem.at[t],
            device_id=dev(z, yp), device_id_type=MESH,
        ).wait_recv()

    c4.wait()
    c5.wait()
    for i in (1, 3, 2):
        q_copy(i).start()

    for n in range(2):
        wait_cell(0, 1 - g, n)
        start_down(0, 1 - g, 0, n)

    def poll(e, _):
        j = e // 2 + 1
        c = (g + e) % 2

        @pl.when((j <= NU) & (z >= j))
        def _():
            slot = up_slot(z, j)
            for n in range(2):
                wait_cell(slot, c, n)
                start_up(slot, c, j, n)

        @pl.when((j <= ND) & ((z + j) % NZ <= KD))
        def _():
            slot = down_slot(z, j)
            for n in range(2):
                wait_cell(slot, c, n)
                start_down(slot, c, j, n)

        r = e // 2

        @pl.when((e % 2 == 0) & (r > 0) & (r < NU))
        def _():
            pl.semaphore_wait(hello.at[r - 1], 2)

        @pl.when((e % 2 == 0) & (r < NU - 1))
        def _():
            for zz in beside:
                pl.semaphore_signal(hello.at[r], inc=1, device_id=dev(zz, y), device_id_type=MESH)

        return 0

    def scores(t, h, k):
        return lax.dot_general(
            qbuf[t, :, h * D : (h + 1) * D], k, (((1,), (1,)), ((), ())), preferred_element_type=jnp.float32
        )

    def weigh(sc, mn):
        mc = mn * LC
        cols = [jnp.exp2(sc[:, n * D : (n + 1) * D] * LC - mc) for n in range(sc.shape[1] // D)]
        return jnp.concatenate(cols, axis=1).astype(jnp.bfloat16)

    def mix(p, ve):
        return lax.dot_general(p, ve, (((1,), (0,)), ((), ())), preferred_element_type=jnp.float32)

    qi = lax.broadcasted_iota(jnp.int32, (R, 2 * R), 0)
    ki = lax.broadcasted_iota(jnp.int32, (R, 2 * R), 1)

    def attend_own(t):
        k = kbuf[0 : 2 * R, :]
        ve = jnp.concatenate([vbuf[0 : 2 * R, :], ebuf[0 : 2 * R, :]], axis=1)
        ok = ki + b * 2 * R <= qi + t * R
        sc = [jnp.where(ok, scores(t, h, k), LOW) for h in range(HG)]
        for h in range(HG):
            mn = jnp.broadcast_to(jnp.max(sc[h], axis=1, keepdims=True), (R, D))
            m_ref[t, h] = mn
            acc_ref[t, h] = mix(weigh(sc[h], mn), ve)

    def attend(t, base, n):
        rows = pl.ds(pl.multiple_of(base, 2 * R), n * 2 * R)
        k = kbuf[rows, :]
        ve = jnp.concatenate([vbuf[rows, :], ebuf[rows, :]], axis=1)
        sc = [scores(t, h, k) for h in range(HG)]
        for h in range(HG):
            mo = m_ref[t, h]
            mn = jnp.maximum(mo, jnp.max(sc[h], axis=1, keepdims=True))
            al = jnp.exp2((mo - mn) * LC)
            pv = mix(weigh(sc[h], mn), ve)
            acc_ref[t, h] = acc_ref[t, h] * jnp.concatenate([al, al], axis=1) + pv
            m_ref[t, h] = mn

    def have(j):
        ups = jnp.minimum(jnp.minimum(j, NU), z)
        return ups + jnp.maximum(0, jnp.minimum(j, ND) - (NZ - z) + 1)

    def item(it, e):
        row = pick(it, [a + 4 * (p + 4 * (j0 + 16 * j1)) for a, j0, j1, p in PLAN])
        gi, polls, j0, j1 = row % 4, row // 4 % 4, row // 16 % 16, row // 256
        gi = jnp.where((gi % 2 == 1) & (g == 0), 4 - gi, gi)
        t = (y + gi) % NY

        @pl.when(j1 == 0)
        def _():
            @pl.when(gi > 0)
            def _():
                wait_q(t)

            attend_own(t)

        before = have(j0)
        count = have(j1) - before
        for n in range(1, 5):

            @pl.when((j1 > 0) & (count == n))
            def _():
                attend(t, (before + 1) * 2 * R, n)

        lax.fori_loop(e, e + polls, poll, 0)
        return e + polls

    lax.fori_loop(0, len(PLAN), item, 0)

    lane1 = lax.broadcasted_iota(jnp.int32, (R, D), 1)

    def stats(t, _):
        x, m = jnp.ones((R, D), jnp.float32), jnp.zeros((R, D), jnp.float32)
        for h in range(HG):
            x = jnp.where((lane1 == h) | (lane1 == 64 + h), acc_ref[t, h, :, D : 2 * D], x)
            m = jnp.where(lane1 == h, m_ref[t, h], m)
        frac = x / pltpu.roll(x, 64, 1)
        xs_ref[...] = jnp.where(lane1 < 64, m * SCALE + jnp.log(x), frac).T
        xrecv[y, t, 0:8] = xs_ref[0:8, :]
        xrecv[y, t, 8:16] = xs_ref[64:72, :]
        return 0

    lax.fori_loop(0, NY, stats, 0)

    def tell(i):
        return pltpu.make_async_remote_copy(
            src_ref=xrecv.at[y], dst_ref=xrecv.at[y], send_sem=ss_sem, recv_sem=sr_sem,
            device_id=dev(z, (y + i) % NY), device_id_type=MESH,
        )

    def back(i):
        return pltpu.make_async_remote_copy(
            src_ref=osend.at[i], dst_ref=orecv.at[y], send_sem=os_sem, recv_sem=or_sem,
            device_id=dev(z, (y + i) % NY), device_id_type=MESH,
        )

    for i in (2, 1, 3):
        tell(i).start()

    def outputs(i, ref, at):
        t = (y + i) % NY
        for h in range(HG):
            inv = 1.0 / jnp.broadcast_to(acc_ref[t, h, :, D : D + 1], (R, D))
            ref[at, :, h * D : (h + 1) * D] = (acc_ref[t, h, :, 0:D] * inv).astype(jnp.bfloat16)

    for i in (2, 3, 1):
        outputs(i, osend, i)
    for i in (2, 3, 1):
        back(i).start()
    outputs(0, orecv, y)

    def landed(ref, sem):
        pltpu.make_async_remote_copy(
            src_ref=ref, dst_ref=ref, send_sem=xk_sem, recv_sem=sem, device_id=dev(z, yp), device_id_type=MESH
        ).wait_recv()

    landed(xrecv.at[0 : NY - 1], sr_sem)

    def join(gg, t):
        xa, xb = xrecv[gg, t], xrecv[2 + gg, t]
        la, lb = xa[0:8], xb[0:8]
        top = jnp.maximum(la, lb)
        ea, eb = jnp.exp(la - top), jnp.exp(lb - top)
        tot = ea + eb
        wa, wb = ea / tot, eb / tot
        pos = (z * NY + t) * R + lax.broadcasted_iota(jnp.int32, (8, D), 1)
        live = pos < len_ref[0]
        lse = jnp.where(live, top + jnp.log(tot), 0.0)
        mass = jnp.where(live, wa * xa[8:16] + wb * xb[8:16], 0.0)
        return lse, mass, jnp.where(live, wa, 0.0), jnp.where(live, wb, 0.0)

    pk_ref[...] = jnp.zeros_like(pk_ref)
    for gg in range(2):
        lse, mass = jnp.zeros((8, D), jnp.float32), jnp.zeros((8, D), jnp.float32)
        for t in range(NY):
            more = join(gg, t)
            lse, mass = lse + more[0], mass + more[1]
        pk_ref[gg * HG : (gg + 1) * HG, :] = lse[0:HG]
        pk_ref[16 + gg * HG : 16 + (gg + 1) * HG, :] = mass[0:HG]
        lse, mass, wa, wb = join(gg, y)
        lse_ref[gg * HG : (gg + 1) * HG, :] = lse[0:HG]
        mass_ref[gg * HG : (gg + 1) * HG, :] = mass[0:HG]
        pk_ref[32 + 16 * gg : 40 + 16 * gg, :] = wa
        pk_ref[40 + 16 * gg : 48 + 16 * gg, :] = wb
    xs_ref[...] = pk_ref[...].T
    zsum[z] = jnp.broadcast_to(jnp.sum(xs_ref[...], axis=0, keepdims=True), (8, D))

    def sum_z(i):
        return pltpu.make_async_remote_copy(
            src_ref=zsum.at[z], dst_ref=zsum.at[z], send_sem=zs_sem, recv_sem=zr_sem,
            device_id=dev((z + i) % NZ, y), device_id_type=MESH,
        )

    def sum_z_start(i, _):
        sum_z(i).start()
        return 0

    lax.fori_loop(1, NZ, sum_z_start, 0)

    landed(orecv.at[0 : NY - 1], or_sem)
    for gg in range(2):
        for h in range(HG):
            at = 32 + 16 * gg + h
            cols = slice(h * D, (h + 1) * D)
            o = xs_ref[:, at : at + 1] * orecv[gg, :, cols].astype(jnp.float32)
            o = o + xs_ref[:, at + 8 : at + 9] * orecv[2 + gg, :, cols].astype(jnp.float32)
            obuf[:, gg * CW + h * D : gg * CW + (h + 1) * D] = o.astype(jnp.bfloat16)
    places = (
        (obuf, out_hbm), (lse_ref, lse_hbm), (mass_ref, mass_hbm), (hl_ref, hl_hbm), (hs_ref, hs_hbm)
    )
    home = [pltpu.make_async_copy(a, o, loc_sem.at[n]) for n, (a, o) in enumerate(places)]
    for d in home[0:3]:
        d.start()

    landed(zsum.at[0 : NZ - 1], zr_sem)
    total = zsum[0]
    for i in range(1, NZ):
        total = total + zsum[i]
    mean = total[0:1, :] / len_ref[0].astype(jnp.float32)
    hl_ref[...] = mean[:, 0 : 2 * HG]
    hs_ref[...] = mean[:, 16 : 16 + 2 * HG]

    for d in home[3:5]:
        d.start()

    def left(ref, sem):
        pltpu.make_async_remote_copy(
            src_ref=ref, dst_ref=ref, send_sem=sem, recv_sem=xk_sem, device_id=dev(z, yp), device_id_type=MESH
        ).wait_send()

    for j in range(NU):

        @pl.when((z < NZ - 1) & (z >= j))
        def _():
            left(kbuf.at[0 : 4 * R, :], us_sem.at[j])

    for j in range(ND):

        @pl.when((z + j) % NZ <= KD)
        def _():
            left(kbuf.at[0 : 4 * R, :], ds_sem.at[j])

    left(kbuf.at[0 : 2 * R, :], xk_sem)
    left(qbuf.at[0 : NY - 1], qs_sem)
    left(xrecv.at[0 : NY - 1], ss_sem)
    left(osend.at[0 : NY - 1], os_sem)
    left(zsum.at[0 : NZ - 1], zs_sem)
    for d in home:
        d.wait()


def hand_on(*refs):
    n = (len(refs) - 2) // 3
    ins, outs, held = refs[:n], refs[n : 2 * n], refs[2 * n : 3 * n]
    come, go = refs[3 * n :]
    for i in range(n):
        pltpu.make_async_copy(ins[i], held[i], come.at[i]).start()
    for i in range(n):
        pltpu.make_async_copy(ins[i], held[i], come.at[i]).wait()
        pltpu.make_async_copy(held[i], outs[i], go.at[i]).start()
    for i in range(n):
        pltpu.make_async_copy(held[i], outs[i], go.at[i]).wait()


def body(queries, keys, values, doc_length, sink_pos):
    NZ = lax.axis_size("seq") // NY
    NU = NZ // 2
    cells = NZ + NU
    f32, bf16 = jnp.float32, jnp.bfloat16
    vm, dma = pltpu.VMEM, pltpu.SemaphoreType.DMA
    results = (
        jax.ShapeDtypeStruct((R, 2 * CW), bf16),
        jax.ShapeDtypeStruct((2 * HG, R), f32),
        jax.ShapeDtypeStruct((2 * HG, R), f32),
        jax.ShapeDtypeStruct((1, 2 * HG), f32),
        jax.ShapeDtypeStruct((1, 2 * HG), f32),
    )
    parts = pl.pallas_call(
        functools.partial(kernel, NZ),
        out_shape=results,
        in_specs=[
            pl.BlockSpec(memory_space=pl.ANY),
            pl.BlockSpec(memory_space=pl.ANY),
            pl.BlockSpec(memory_space=pl.ANY),
            pl.BlockSpec(memory_space=pl.ANY),
            pl.BlockSpec(memory_space=pl.ANY),
        ],
        out_specs=(pl.BlockSpec(memory_space=pl.ANY),) * 5,
        scratch_shapes=[
            pltpu.SMEM((1,), jnp.int32),
            pltpu.SMEM((4,), jnp.int32),
            vm((2 * HG, R), f32),
            vm((2 * HG, R), f32),
            vm((1, 2 * HG), f32),
            vm((1, 2 * HG), f32),
            vm((NY, R, CW), bf16),
            vm((R, CW), bf16),
            vm((cells * 2 * R, D), bf16),
            vm((cells * 2 * R, D), bf16),
            vm((R, D), bf16),
            vm((R, D), bf16),
            vm((NZ * 2 * R, D), bf16),
            vm((NY, HG, R, D), f32),
            vm((NY, HG, R, 2 * D), f32),
            vm((NY, R, CW), bf16),
            vm((NY, R, CW), bf16),
            vm((R, 2 * CW), bf16),
            vm((NY, NY, 16, R), f32),
            vm((D, R), f32),
            vm((D, R), f32),
            vm((NZ, 8, D), f32),
            dma((8,)),
            dma,
            dma((NY,)),
            dma,
            dma((cells, 2)),
            dma((cells, 2)),
            dma((NU,)),
            dma((NU,)),
            dma,
            dma,
            dma,
            dma,
            dma,
            dma,
            pltpu.SemaphoreType.REGULAR((NU - 1,)),
        ],
        compiler_params=pltpu.CompilerParams(
            collective_id=0, has_side_effects=True, vmem_limit_bytes=56 * 2**20
        ),
    )(doc_length, sink_pos, queries, keys, values)
    out, lse, mass, hl, hs = pl.pallas_call(
        hand_on,
        out_shape=results,
        in_specs=[pl.BlockSpec(memory_space=pl.ANY)] * 5,
        out_specs=(pl.BlockSpec(memory_space=pl.ANY),) * 5,
        scratch_shapes=[vm(r.shape, r.dtype) for r in results] + [dma((5,)), dma((5,))],
    )(*parts)
    return out, lse, mass, hl.reshape(2 * HG), hs.reshape(2 * HG)


def solution(mesh):
    rows = P(("doc", "seq"), None)
    return jax.shard_map(
        body,
        mesh=mesh,
        in_specs=(rows, rows, rows, P("doc"), P("doc")),
        out_specs=(rows, P(None, ("doc", "seq")), P(None, ("doc", "seq")), P("doc"), P("doc")),
        check_vma=False,
    )
```
